32 devices in a mesh: seq: 8 (over y, x, core), batch: 4 (over z).
Axes of the slice: x: 2, y: 2, z: 4, core: 2. Of those that a mesh axis runs over, the one named last changes fastest.
Arguments:
- queries: bfloat16 [4096, 4096], P(('batch', 'seq')), parts along dimension 0, may hold values from -6 to 6
- key_vectors: bfloat16 [4096, 4096], P(('batch', 'seq')), parts along dimension 0, may hold values from -6 to 6
- value_vectors: bfloat16 [4096, 4096], P(('batch', 'seq')), parts along dimension 0, may hold values from -6 to 6
- residual_in: bfloat16 [4096, 4096], P(('batch', 'seq')), parts along dimension 0, may hold values from -6 to 6
- input_logit: float32 [8, 4096], P(None, ('batch', 'seq')), parts along dimension 1, may hold values from -8 to 300
- forget_logit: float32 [8, 4096], P(None, ('batch', 'seq')), parts along dimension 1, may hold values from -3 to 13
- mix_gain: float32 [4096], replicated, may hold values from 0.1 to 1.9
- ffn_gain: float32 [4096], replicated, may hold values from 0.1 to 1.9
- expert_gate: bfloat16 [8, 4096, 704], P('seq'), may hold values from -0.09375 to 0.09375
- expert_up: bfloat16 [8, 4096, 704], P('seq'), may hold values from -0.09375 to 0.09375
- expert_down: bfloat16 [8, 704, 4096], P('seq'), may hold values from -0.21875 to 0.21875
- routes: int32 [4096, 2], P(('batch', 'seq')), parts along dimension 0, may hold values from 0 to 7, all different within a row; in each aligned block of 128 rows (0 to 127, 128 to 255, ...) at most 64 rows name the same one
- route_weight: float32 [4096, 2], P(('batch', 'seq')), parts along dimension 0, may hold values from 0.2 to 1
Outputs:
- block_out: bfloat16 [4096, 4096], P(('batch', 'seq')), parts along dimension 0
The draws below stay inside these ranges and needn't reach their ends.
There are 4 independent parts, one for each index of `batch`. The reference program is written for one: setup_inputs(seed, part) draws one part's arguments, and reference() takes and returns one part's arrays. A program takes and returns all parts, laid end to end along the dimension named above; an argument that names none is the same for every part. Nothing has to cross between parts.
Inputs may be any that keep to these rules, and one draw needn't show every extreme that they name: `routes`: each row names two different experts. Within the rows of one device no expert is named by more than 64 rows, and in some device one expert is named by exactly 64 rows.
All inputs are finite; a program needn't handle non-finite values.
Results may differ from the reference program's by a relative error of at most 0.0081.
Values may be sent and summed in bfloat16 or wider, within the bound.
A program may use at most 128 MiB of HBM per device.

```python
import math
import jax
import jax.numpy as jnp
import numpy as np
from jax import lax

MIXER_HEADS = 8
DH = 512
D = 4096
FF = 704
TOK_DEV = 128
SEQUENCE_LENGTH = 1024
EXPERTS = 8
CAP = 64


def draw_forget_logit(key, part):
    random_child_keys = jax.random.split(jax.random.fold_in(key, 11), 6)
    chooser = jax.random.uniform(random_child_keys[0], (MIXER_HEADS, 1))
    quick_head = chooser < 0.5
    horizon = TOK_DEV * jax.random.uniform(random_child_keys[1], (MIXER_HEADS, 1), minval=0.15, maxval=0.25)
    slow_rate = jnp.log(1.0 / 0.7) / SEQUENCE_LENGTH * jnp.ones((MIXER_HEADS, 1), jnp.float32)
    base_rate = jnp.where(quick_head, 1.0 / horizon, slow_rate)
    blocks = SEQUENCE_LENGTH // TOK_DEV
    device_factor = jnp.exp(jax.random.uniform(random_child_keys[2], (MIXER_HEADS, blocks), minval=-0.7, maxval=0.7))
    device_factor = jnp.repeat(device_factor, TOK_DEV, axis=1)
    roughness = jax.random.uniform(random_child_keys[3], (MIXER_HEADS, SEQUENCE_LENGTH), minval=0.5, maxval=1.5)
    forget_decay_speed = base_rate * device_factor * roughness
    spike_locations = jax.random.randint(random_child_keys[4], (3,), 0, SEQUENCE_LENGTH)
    spike_present = jnp.any(jnp.arange(SEQUENCE_LENGTH)[None, :] == spike_locations[:, None], axis=0)[None, :]
    spike_frequency = jax.random.uniform(random_child_keys[5], (MIXER_HEADS, SEQUENCE_LENGTH), minval=0.22, maxval=0.69)
    forget_decay_speed = jnp.where(spike_present, spike_frequency, forget_decay_speed)
    return jnp.log(1.0 / jnp.expm1(forget_decay_speed)).astype(jnp.float32)


def draw_input_logit(key, part):
    random_child_keys = jax.random.split(jax.random.fold_in(key, 23), 5)
    drawn = jax.random.normal(random_child_keys[4], (MIXER_HEADS, SEQUENCE_LENGTH)) * 1.5 - 1.0
    return jnp.clip(drawn, -8.0, 8.0).astype(jnp.float32)


def block_levels(rng, dims, shards, least, largest):
    def one(dim, blocks):
        draws = jax.random.uniform(jax.random.fold_in(jax.random.fold_in(rng, 6), dim), (blocks,), jnp.float32, least / len(shards), largest / len(shards))
        return jnp.repeat(jnp.exp(draws), dims[dim] // blocks).reshape((-1,) + (1,) * (len(dims) - dim - 1))

    gain = one(*shards[0])
    for cut in shards[1:]:
        gain = gain * one(*cut)
    return gain


def shared_out(key, own, number, rows, number_of, top, reach, lean):
    sequence = jax.random.permutation(key, number_of)
    crowded, common = portions_of(number_of, rows * top, reach, lean, True), portions_of(number_of, rows * top, reach, lean, False)
    places = jnp.arange(number_of)

    def named(sizes, turn):
        used = int((sizes > 0).sum())
        fixed = max(1, used // 4)
        shifted = fixed + (places - fixed + turn * (used - fixed)) % max(1, number_of - fixed)
        return jnp.zeros((number_of,), jnp.int32).at[sequence[jnp.where(places < fixed, places, shifted)]].set(jnp.asarray(sizes, jnp.int32))

    sizes = jnp.where(number % 4 == 0, named(crowded, number // 4), named(common, number - number // 4 - 1))
    mixed = jax.random.permutation(jax.random.fold_in(own, 3), number_of)
    donor, receiver = mixed[0:number_of // 2 * 2:2], mixed[1:number_of // 2 * 2:2]
    slack = jnp.minimum(sizes[donor] - 1, reach - sizes[receiver]) // 2
    slack = jnp.where((donor == sequence[0]) | (receiver == sequence[0]) | (sizes[receiver] == 0), 0, jnp.maximum(slack, 0))
    shifted = jax.random.randint(jax.random.fold_in(own, 4), (number_of // 2,), 0, 1 << 20) % (slack + 1)
    sizes = sizes.at[donor].add(-shifted).at[receiver].add(shifted)
    members = jnp.searchsorted(jnp.cumsum(sizes), jnp.arange(rows * top), side="right").astype(jnp.int32)
    grid = members.reshape(top, rows).T
    grid = grid[jax.random.permutation(jax.random.fold_in(own, 1), rows)]
    turn = jax.random.randint(jax.random.fold_in(own, 2), (rows, 1), 0, top)
    return jnp.take_along_axis(grid, (jnp.arange(top)[None, :] + turn) % top, axis=1)


def portions_of(amount, total, limit, skew, full):
    weights = [(1 << 20) // math.isqrt(standing ** skew) + 1 for standing in range(1, amount + 1)]
    largest = limit if full else min(limit, max(-(-total // amount), total * weights[0] // sum(weights)))
    least = 1 if total - largest >= amount - 1 else 0
    given, surplus = [largest] + [least] * (amount - 1), total - largest - least * (amount - 1)
    while surplus > 0:
        free = [i for i in range(1, amount) if given[i] < largest] or [i for i in range(1, amount) if given[i] < limit]
        whole, remaining = sum([weights[i] for i in free]), surplus
        for i in free:
            more = min(limit - given[i], max(1, remaining * weights[i] // whole), surplus)
            given[i] = given[i] + more
            surplus = surplus - more
    return np.array(given)


def scatter_about(own_key, extent, spread, bound, cuts=(), kind=jnp.bfloat16):
    entries = spread * jax.random.normal(own_key, extent, jnp.float32)
    if cuts:
        entries = entries * block_levels(own_key, extent, cuts, -0.22, 0.18)
    return jnp.clip(entries, -bound, bound).astype(kind)


def setup_inputs(seed: int = 0, part: int = 0) -> dict:
    seeds = jax.random.split(jax.random.key(seed), 14)
    own_keys = jax.random.split(jax.random.fold_in(seeds[13], part), 14)
    queries = scatter_about(own_keys[0], (SEQUENCE_LENGTH, D), 1.0, 6.0, ((0, 8),))
    key_vectors = scatter_about(own_keys[1], (SEQUENCE_LENGTH, D), 1.0, 6.0, ((0, 8),))
    value_vectors = scatter_about(own_keys[2], (SEQUENCE_LENGTH, D), 1.0, 6.0, ((0, 8),))
    residual_in = scatter_about(own_keys[3], (SEQUENCE_LENGTH, D), 1.0, 6.0, ((0, 8),))
    input_logit = draw_input_logit(jax.random.fold_in(jax.random.fold_in(seeds[13], part), 71), part)
    forget_logit = draw_forget_logit(jax.random.fold_in(jax.random.fold_in(seeds[13], part), 71), part)
    mix_gain = jnp.clip(1.0 + 0.18 * jax.random.normal(seeds[6], (D,), jnp.float32), 0.1, 1.9)
    ffn_gain = jnp.clip(1.0 + 0.18 * jax.random.normal(seeds[7], (D,), jnp.float32), 0.1, 1.9)
    expert_gate = scatter_about(seeds[8], (EXPERTS, D, FF), D ** -0.5, 0.09375, ((0, 8),))
    expert_up = scatter_about(seeds[9], (EXPERTS, D, FF), D ** -0.5, 0.09375, ((0, 8),))
    expert_down = scatter_about(seeds[10], (EXPERTS, FF, D), FF ** -0.5, 0.21875, ((0, 8),))
    routes_keys = jax.random.split(jax.random.fold_in(own_keys[11], 1), SEQUENCE_LENGTH // TOK_DEV)
    routes_turns = jax.random.permutation(jax.random.fold_in(own_keys[11], 3), SEQUENCE_LENGTH // TOK_DEV)
    routes = jax.vmap(lambda own, number: shared_out(jax.random.fold_in(own_keys[11], 2), own, number, TOK_DEV, EXPERTS, 2, CAP, 2))(routes_keys, routes_turns).reshape((SEQUENCE_LENGTH, 2))
    route_weight = jnp.clip(0.2 + 0.8 * jax.random.uniform(own_keys[12], (SEQUENCE_LENGTH, 2), jnp.float32) ** block_levels(own_keys[12], (SEQUENCE_LENGTH, 2), ((0, 8),), -0.2, 0.2), 0.2, 1.0)
    return dict(queries=queries, key_vectors=key_vectors, value_vectors=value_vectors, residual_in=residual_in, input_logit=input_logit, forget_logit=forget_logit, mix_gain=mix_gain, ffn_gain=ffn_gain, expert_gate=expert_gate, expert_up=expert_up, expert_down=expert_down, routes=routes, route_weight=route_weight)


NEG_FILL = -1e+30
EPSILON = 1e-06

def join_states(earlier, later):
    total_early, state_early, normv_early, peak_early = earlier
    total_late, state_late, normv_late, peak_late = later
    carried = total_late + peak_early
    peak_new = jnp.maximum(carried, peak_late)
    scale_early = jnp.exp(carried - peak_new)
    scale_late = jnp.exp(peak_late - peak_new)
    state_new = scale_early[..., None] * state_early + scale_late[..., None] * state_late
    normv_new = scale_early * normv_early + scale_late * normv_late
    return (total_early + total_late, state_new, normv_new, peak_new)

def block_summary(keys_three, values_three, log_forget, input_gate):
    cumul_log = jnp.cumsum(log_forget, axis=1)
    tail_log = cumul_log[:, -1:] - cumul_log + input_gate
    peak_log = lax.optimization_barrier(jnp.max(tail_log, axis=1))
    weight = jnp.exp(tail_log - peak_log[:, None])
    weighted = keys_three.astype(jnp.float32) * jnp.transpose(weight)[:, :, None]
    rounded = lax.optimization_barrier(weighted.astype(jnp.bfloat16))
    state_mat = jnp.einsum('thd,the->hde', rounded.astype(jnp.float32), values_three.astype(jnp.float32))
    norm_vec = lax.optimization_barrier(jnp.sum(weighted, axis=0))
    total_log = jnp.broadcast_to(cumul_log[:, -1:], norm_vec.shape)
    peak_full = jnp.broadcast_to(peak_log[:, None], norm_vec.shape)
    return (total_log, state_mat, norm_vec, peak_full)

def block_output(queries_three, keys_three, values_three, log_forget, input_gate, carry_in):
    length_block = queries_three.shape[0]
    inverse_root = 1.0 / math.sqrt(queries_three.shape[2])
    cumul_log = jnp.cumsum(log_forget, axis=1)
    log_weight = cumul_log[:, :, None] - cumul_log[:, None, :] + input_gate[:, None, :]
    causal = jnp.arange(length_block)[:, None] >= jnp.arange(length_block)[None, :]
    log_weight = jnp.where(causal[None], log_weight, NEG_FILL)
    carry_total, carry_state, carry_norm, carry_peak = carry_in
    carried = cumul_log + carry_peak[:, 0:1]
    peak_log = jnp.maximum(lax.optimization_barrier(jnp.max(log_weight, axis=2)), carried)
    decay_mat = jnp.exp(log_weight - peak_log[:, :, None])
    query_float = queries_three.astype(jnp.float32)
    scores = jnp.einsum('thd,shd->hts', query_float, keys_three.astype(jnp.float32)) * inverse_root
    coef = decay_mat * scores
    denom_sum = lax.optimization_barrier(jnp.sum(coef, axis=2))
    coef_round = lax.optimization_barrier(coef.astype(jnp.bfloat16))
    numer_sum = jnp.einsum('hts,she->the', coef_round.astype(jnp.float32), values_three.astype(jnp.float32))
    carry_reach = jnp.exp(carried - peak_log) * inverse_root
    from_state = jnp.einsum('thd,hde->the', query_float, carry_state, precision=lax.Precision.HIGHEST)
    from_norm = jnp.einsum('thd,hd->ht', query_float, carry_norm, precision=lax.Precision.HIGHEST)
    numer_sum = numer_sum + jnp.transpose(carry_reach)[:, :, None] * from_state
    denom_sum = denom_sum + carry_reach * from_norm
    floor_sum = jnp.maximum(jnp.abs(denom_sum), 1.0)
    return numer_sum / jnp.transpose(floor_sum)[:, :, None]

def reference(queries, key_vectors, value_vectors, residual_in, input_logit, forget_logit, mix_gain, ffn_gain, expert_gate, expert_up, expert_down, routes, route_weight):
    log_forget = jax.nn.log_sigmoid(forget_logit)
    blocks = SEQUENCE_LENGTH // TOK_DEV

    def split_rows(array):
        return array.reshape(blocks, TOK_DEV, MIXER_HEADS, DH)

    def split_gates(array):
        return jnp.transpose(array.reshape(MIXER_HEADS, blocks, TOK_DEV), (1, 0, 2))
    initial = (jnp.zeros((MIXER_HEADS, DH), jnp.float32), jnp.zeros((MIXER_HEADS, DH, DH), jnp.float32), jnp.zeros((MIXER_HEADS, DH), jnp.float32), jnp.full((MIXER_HEADS, DH), NEG_FILL, jnp.float32))

    def advance(carry_in, pieces):
        query_block, key_block, value_block, forget_block, input_block = pieces
        result = block_output(query_block, key_block, value_block, forget_block, input_block, carry_in)
        carry_out = join_states(carry_in, block_summary(key_block, value_block, forget_block, input_block))
        return (carry_out, result)
    unused, mixer_out = lax.scan(advance, initial, (split_rows(queries), split_rows(key_vectors), split_rows(value_vectors), split_gates(log_forget), split_gates(input_logit)))
    mixer_out = mixer_out.reshape(SEQUENCE_LENGTH, D)
    mixer_square = lax.optimization_barrier(jnp.mean(mixer_out * mixer_out, axis=1, keepdims=True))
    updated = (residual_in.astype(jnp.float32) + mixer_out * lax.rsqrt(mixer_square + EPSILON) * mix_gain).astype(jnp.bfloat16)
    updated_float = updated.astype(jnp.float32)
    updated_square = lax.optimization_barrier(jnp.mean(updated_float * updated_float, axis=1, keepdims=True))
    normed = (updated_float * lax.rsqrt(updated_square + EPSILON) * ffn_gain).astype(jnp.bfloat16)
    flat_routes = routes.reshape(blocks, 2 * TOK_DEV)
    matches = (flat_routes[:, :, None] == jnp.arange(EXPERTS, dtype=jnp.int32)[None, None, :]).astype(jnp.int32)
    before = jnp.cumsum(matches, axis=1) - matches
    position = lax.optimization_barrier(jnp.sum(before * matches, axis=2))
    source_index = jnp.arange(blocks, dtype=jnp.int32)[:, None]
    slot_index = (flat_routes * (blocks * CAP) + source_index * CAP + position).reshape(SEQUENCE_LENGTH, 2).astype(jnp.int32)
    buffer_rows = jnp.zeros((EXPERTS * blocks * CAP, D), jnp.bfloat16)
    buffer_rows = buffer_rows.at[slot_index[:, 0]].set(normed).at[slot_index[:, 1]].set(normed)

    def run_expert(pieces):
        row_block, gate_weight, up_weight, down_weight = pieces
        gate_val = jnp.dot(row_block, gate_weight, preferred_element_type=jnp.float32)
        up_val = jnp.dot(row_block, up_weight, preferred_element_type=jnp.float32)
        hidden = (jax.nn.silu(gate_val) * up_val).astype(jnp.bfloat16)
        return jnp.dot(hidden, down_weight, preferred_element_type=jnp.float32).astype(jnp.bfloat16)
    outputs = lax.map(run_expert, (buffer_rows.reshape(EXPERTS, blocks * CAP, D), expert_gate, expert_up, expert_down)).reshape(EXPERTS * blocks * CAP, D)
    first_out = outputs[slot_index[:, 0]].astype(jnp.float32)
    second_out = outputs[slot_index[:, 1]].astype(jnp.float32)
    expert_mix = route_weight[:, 0:1] * first_out + route_weight[:, 1:2] * second_out
    return (updated_float + expert_mix).astype(jnp.bfloat16)
```

```python
import functools
import math

import jax
import jax.numpy as jnp
from jax import lax
from jax.experimental import pallas as pl
from jax.experimental.pallas import tpu as pltpu
from jax.sharding import PartitionSpec as P

EPSILON = 1e-06
CHUNKS = 4
HALVES = 2
FLIPS = (6, 4, 2, 7, 5, 3, 1)
SLOT_ORDER = (0, 2, 4, 6, 1, 3, 5, 7)
VMEM_BYTES = 67043328
LOW = -1e30


def exchange_kernel(moves, devices, *refs):
    count = len(moves)
    sources, targets = refs[:count], refs[count : 2 * count]
    send_sem, recv_sem, local_sem = refs[2 * count :]
    me = lax.axis_index("seq")
    others = [lax.rem(me + step, devices) for step in range(1, devices)]
    barrier = pltpu.get_barrier_semaphore()
    for other in others:
        pl.semaphore_signal(
            barrier, inc=1, device_id={"seq": other}, device_id_type=pl.DeviceIdType.MESH
        )
    pl.semaphore_wait(barrier, devices - 1)
    copies = []
    for i, (take, put) in enumerate(moves):
        for step, other in enumerate(others):
            copies.append(
                pltpu.make_async_remote_copy(
                    src_ref=take(sources[i], other),
                    dst_ref=put(targets[i], me),
                    send_sem=send_sem.at[i, step],
                    recv_sem=recv_sem.at[i, step],
                    device_id={"seq": other},
                    device_id_type=pl.DeviceIdType.MESH,
                )
            )
            copies[-1].start()
    for i, (take, put) in enumerate(moves):
        copies.append(
            pltpu.make_async_copy(take(sources[i], me), put(targets[i], me), local_sem.at[i])
        )
        copies[-1].start()
    for copy in copies:
        copy.wait()


def exchange(moves, devices, number, sources, shapes):
    far = pl.BlockSpec(memory_space=pl.ANY)
    count = len(moves)
    return pl.pallas_call(
        functools.partial(exchange_kernel, moves, devices),
        out_shape=shapes,
        in_specs=[far] * count,
        out_specs=[far] * count,
        scratch_shapes=[
            pltpu.SemaphoreType.DMA((count, devices - 1)),
            pltpu.SemaphoreType.DMA((count, devices - 1)),
            pltpu.SemaphoreType.DMA((count,)),
        ],
        compiler_params=pltpu.CompilerParams(collective_id=number, has_side_effects=True),
    )(*sources)


def head_mix(query, key, value, input_gate, forget_gate):
    positions, head_dim = query.shape
    cumul_log = jnp.cumsum(jax.nn.log_sigmoid(forget_gate))
    level = input_gate - cumul_log
    top = lax.cummax(level, axis=0)
    scores = lax.dot_general(
        query, key, (((1,), (1,)), ((), ())), preferred_element_type=jnp.float32
    )
    causal = jnp.arange(positions)[:, None] >= jnp.arange(positions)[None, :]
    decay = jnp.exp(jnp.minimum(level[None, :] - top[:, None], 0.0))
    coef = jnp.where(causal, decay * scores, 0.0) * (1.0 / math.sqrt(head_dim))
    denom_sum = jnp.sum(coef, axis=1, keepdims=True)
    numer_sum = jnp.dot(coef.astype(jnp.bfloat16), value, preferred_element_type=jnp.float32)
    return numer_sum / jnp.maximum(jnp.abs(denom_sum), 1.0)


def fused_kernel(
    query_far,
    key_far,
    value_far,
    residual_far,
    input_gate,
    forget_gate,
    routes,
    weights,
    mix_gain,
    ffn_gain,
    gate_far,
    up_far,
    down_far,
    out,
    info,
    gates,
    level,
    top,
    slot_weight,
    query_all,
    key_all,
    value_all,
    mixed,
    mixer_in,
    residual,
    updated,
    rows,
    gate,
    up,
    down,
    gate_sum,
    up_sum,
    hidden,
    own,
    core_out,
    core_in,
    hop_out,
    hop_in,
    keep,
    last_out,
    last_in,
    load_sem,
    info_send,
    info_recv,
    key_send,
    key_recv,
    value_send,
    value_recv,
    query_send,
    query_recv,
    mixed_send,
    mixed_recv,
    gather_send,
    gather_recv,
    core_send,
    core_recv,
    hop_send,
    hop_recv,
    last_send,
    last_recv,
):
    me = lax.axis_index("seq")
    heads, tokens = input_gate.shape
    devices = heads
    head_dim = key_all.shape[1]
    part = tokens // CHUNKS
    width = out.shape[1] // HALVES
    four = devices // 2 * part

    def peer(flip):
        total = 0
        for bit in (1, 2, 4):
            own_bit = lax.rem(lax.div(me, bit), 2)
            total = total + bit * ((1 - own_bit) if flip & bit else own_bit)
        return total

    started = []

    def remote(source, target, send_sem, recv_sem, flip):
        copy = pltpu.make_async_remote_copy(
            src_ref=source,
            dst_ref=target,
            send_sem=send_sem,
            recv_sem=recv_sem,
            device_id={"seq": peer(flip)},
            device_id_type=pl.DeviceIdType.MESH,
        )
        started.append(copy)
        copy.start()
        return copy

    def block_rows(origin, count):
        return pl.ds(pl.multiple_of(origin * count, count), count)

    def head_columns(origin):
        return pl.ds(pl.multiple_of(origin * head_dim, head_dim), head_dim)

    loads = [
        pltpu.make_async_copy(source, target, load_sem.at[i])
        for i, (source, target) in enumerate(
            (
                (key_far.at[:, head_columns(me)], key_all.at[block_rows(me, tokens), :]),
                (value_far.at[:, head_columns(me)], value_all.at[block_rows(me, tokens), :]),
                (residual_far, residual),
                (gate_far, gate),
                (up_far, up),
                (down_far, down),
            )
            + tuple(
                (
                    query_far.at[pl.ds(j * part, part), head_columns(me)],
                    query_all.at[j, block_rows(me, part), :],
                )
                for j in range(CHUNKS)
            )
        )
    ]
    forget = forget_gate[...]
    info[me, 0:8, :] = input_gate[...]
    info[me, 8:16, :] = -(jnp.maximum(-forget, 0.0) + jnp.log1p(jnp.exp(-jnp.abs(forget))))
    info[me, 16:18, :] = routes[...].astype(jnp.float32)
    info[me, 18:20, :] = weights[...]
    barrier = pltpu.get_barrier_semaphore()
    for flip in FLIPS:
        pl.semaphore_signal(
            barrier,
            inc=1,
            device_id={"seq": peer(flip)},
            device_id_type=pl.DeviceIdType.MESH,
        )
    pl.semaphore_wait(barrier, devices - 1)

    infos, keys, values, queries, results = {}, {}, {}, {}, {}
    for flip in FLIPS:
        keys[flip] = remote(
            key_far.at[:, head_columns(peer(flip))],
            key_all.at[block_rows(me, tokens), :],
            key_send.at[flip - 1],
            key_recv.at[flip - 1],
            flip,
        )
        infos[flip] = remote(
            info.at[me], info.at[me], info_send.at[flip - 1], info_recv.at[flip - 1], flip
        )
    for flip in FLIPS:
        values[flip] = remote(
            value_far.at[:, head_columns(peer(flip))],
            value_all.at[block_rows(me, tokens), :],
            value_send.at[flip - 1],
            value_recv.at[flip - 1],
            flip,
        )
    for j in range(CHUNKS):
        for flip in FLIPS:
            queries[j, flip] = remote(
                query_far.at[pl.ds(j * part, part), head_columns(peer(flip))],
                query_all.at[j, block_rows(me, part), :],
                query_send.at[j, flip - 1],
                query_recv.at[j, flip - 1],
                flip,
            )
    for load in loads:
        load.start()

    for flip in FLIPS:
        infos[flip].wait_recv()
    for block in range(devices):
        gates[block : block + 1, :] = info[block, pl.ds(me, 1), :]
        gates[devices + block : devices + block + 1, :] = info[block, pl.ds(heads + me, 1), :]
    across = lax.broadcasted_iota(jnp.int32, (tokens, tokens), 0)
    along = lax.broadcasted_iota(jnp.int32, (tokens, tokens), 1)
    local_sum = jnp.dot(
        gates[devices : 2 * devices, :],
        (across <= along).astype(jnp.float32),
        precision=lax.Precision.HIGHEST,
        preferred_element_type=jnp.float32,
    )
    before = jnp.zeros((1, 1), jnp.float32)
    peak = jnp.full((1, 1), LOW, jnp.float32)
    for block in range(devices):
        line = local_sum[block : block + 1, :]
        level_line = gates[block : block + 1, :] - (line + before)
        before = before + line[:, tokens - 1 : tokens]
        level[:, block * tokens : (block + 1) * tokens] = level_line
        spread = jnp.where(along <= across, jnp.broadcast_to(level_line, (tokens, tokens)), LOW)
        tops = jnp.maximum(jnp.max(spread, axis=1, keepdims=True), peak)
        peak = jnp.maximum(peak, jnp.max(level_line, axis=1, keepdims=True))
        for j in range(CHUNKS):
            top[j, block * part : (block + 1) * part, :] = tops[j * part : (j + 1) * part, :]
    for slot in range(devices):
        told = info.at[peer(slot)] if slot else info.at[me]
        line = jnp.where(told[16:17, :].astype(jnp.int32) == me, told[18:19, :], 0.0) + jnp.where(
            told[17:18, :].astype(jnp.int32) == me, told[19:20, :], 0.0
        )
        spread = jnp.where(along == across, jnp.broadcast_to(line, (tokens, tokens)), 0.0)
        column = jnp.sum(spread, axis=1, keepdims=True)
        place = SLOT_ORDER.index(slot) * part
        for j in range(CHUNKS):
            slot_weight[j, place : place + part, :] = column[j * part : (j + 1) * part, :]

    for flip in FLIPS:
        keys[flip].wait_recv()
        values[flip].wait_recv()
    loads[0].wait()
    loads[1].wait()
    place_in = lax.broadcasted_iota(jnp.int32, (devices * part, 1), 0)
    place_in = lax.shift_right_logical(place_in, part.bit_length() - 1) * (tokens - part) + place_in
    place_key = lax.broadcasted_iota(jnp.int32, (1, devices * tokens), 1)
    for j in range(CHUNKS):
        for flip in FLIPS:
            queries[j, flip].wait_recv()
        loads[6 + j].wait()
        scores = lax.dot_general(
            query_all[j],
            key_all[...],
            (((1,), (1,)), ((), ())),
            preferred_element_type=jnp.float32,
        )
        decay = jnp.exp(jnp.minimum(level[...] - top[j], 0.0))
        coef = jnp.where(place_key <= place_in + j * part, decay * scores, 0.0) * (
            1.0 / math.sqrt(head_dim)
        )
        denom_sum = jnp.sum(coef, axis=1, keepdims=True)
        numer_sum = jnp.dot(
            coef.astype(jnp.bfloat16), value_all[...], preferred_element_type=jnp.float32
        )
        mixed[j] = (numer_sum / jnp.maximum(jnp.abs(denom_sum), 1.0)).astype(jnp.bfloat16)
        for flip in FLIPS:
            results[j, flip] = remote(
                mixed.at[j, block_rows(peer(flip), part), :],
                mixer_in.at[j, :, head_columns(me)],
                mixed_send.at[j, flip - 1],
                mixed_recv.at[j, flip - 1],
                flip,
            )
        mixer_in[j, :, head_columns(me)] = mixed[j, block_rows(me, part), :]

    def slot_rows(slot):
        return pl.ds(SLOT_ORDER.index(slot) * part, part)

    def columns(half):
        return pl.ds(half * width, width)

    gathers = {}

    def gather(j, number, source, target, flip, half=None):
        view = slice(None) if half is None else columns(half)
        gathers[j, number] = remote(
            rows.at[j, slot_rows(source), view],
            rows.at[j, slot_rows(target), view],
            gather_send.at[j, number],
            gather_recv.at[j, number],
            flip,
        )

    def normalise(j):
        for flip in FLIPS:
            results[j, flip].wait_recv()
        if j == 0:
            loads[2].wait()
        span = slice(j * part, (j + 1) * part)
        mixer_out = mixer_in[j].astype(jnp.float32)
        square = jnp.mean(mixer_out * mixer_out, axis=1, keepdims=True)
        value = (
            residual[span, :].astype(jnp.float32)
            + mixer_out * lax.rsqrt(square + EPSILON) * mix_gain[...]
        ).astype(jnp.bfloat16)
        updated[span, :] = value
        value = value.astype(jnp.float32)
        square = jnp.mean(value * value, axis=1, keepdims=True)
        rows[j, 0:part, :] = (value * lax.rsqrt(square + EPSILON) * ffn_gain[...]).astype(
            jnp.bfloat16
        )

    def send_own(j):
        gather(j, 0, 0, 2, 2, 0)
        gather(j, 1, 0, 4, 4, 1)
        gather(j, 2, 0, 2, 2, 1)
        gather(j, 3, 0, 4, 4, 0)
        gather(j, 4, 0, 1, 1)

    def relay(j):
        gathers[j, 0].wait_recv()
        gather(j, 5, 2, 6, 4, 0)
        gathers[j, 1].wait_recv()
        gather(j, 6, 4, 6, 2, 1)
        gathers[j, 2].wait_recv()
        gather(j, 7, 2, 3, 1)
        gathers[j, 3].wait_recv()
        gather(j, 8, 4, 5, 1)

    def relay_last(j):
        gathers[j, 5].wait_recv()
        gathers[j, 6].wait_recv()
        gather(j, 9, 6, 7, 1)

    core_copies, hop_copies, last_copies = {}, {}, {}

    def compute(j):
        for number in (4, 7, 8, 9):
            gathers[j, number].wait_recv()
        if j == 0:
            loads[3].wait()
            loads[4].wait()
        for weight, total in ((gate, gate_sum), (up, up_sum)):
            total[...] = lax.dot_general(
                rows[j],
                weight[...],
                (((1,), (1,)), ((), ())),
                preferred_element_type=jnp.float32,
            )
        gate_val = gate_sum[...]
        hidden[...] = (gate_val / (1.0 + jnp.exp(-gate_val)) * up_sum[...]).astype(jnp.bfloat16)
        if j == 0:
            loads[5].wait()
        for half in range(HALVES):
            terms = (
                jnp.dot(hidden[...], down[:, columns(half)], preferred_element_type=jnp.float32)
                * slot_weight[j]
            ).astype(jnp.bfloat16)
            own[j % 2, half] = terms[:four, :]
            core_out[j, half] = terms[four:, :]
            core_copies[j, half] = remote(
                core_out.at[j, half],
                core_in.at[j, half],
                core_send.at[j, half],
                core_recv.at[j, half],
                1,
            )

    def first_hop(j, half):
        first, second = (2, 4) if half == 0 else (4, 2)
        core_copies[j, half].wait_recv()
        for slot in (6, first, second, 0):
            view = slot_rows(slot)
            both = own[j % 2, half, view, :].astype(jnp.float32) + core_in[
                j, half, view, :
            ].astype(jnp.float32)
            if slot in (0, second):
                keep[j, half, 0 if slot == 0 else 1] = both
                continue
            place = 1 if slot == 6 else 0
            hop_out[j, half, place] = both.astype(jnp.bfloat16)
            hop_copies[j, half, place] = remote(
                hop_out.at[j, half, place],
                hop_in.at[j, half, place],
                hop_send.at[j, half, place],
                hop_recv.at[j, half, place],
                first,
            )

    def second_hop(j, half):
        second = 4 if half == 0 else 2
        hop_copies[j, half, 1].wait_recv()
        last_out[j, half] = (
            keep[j, half, 1] + hop_in[j, half, 1].astype(jnp.float32)
        ).astype(jnp.bfloat16)
        last_copies[j, half] = remote(
            last_out.at[j, half],
            last_in.at[j, half],
            last_send.at[j, half],
            last_recv.at[j, half],
            second,
        )

    def finish(j, half):
        hop_copies[j, half, 0].wait_recv()
        last_copies[j, half].wait_recv()
        span = slice(j * part, (j + 1) * part)
        out[span, columns(half)] = (
            updated[span, columns(half)].astype(jnp.float32)
            + (
                keep[j, half, 0]
                + hop_in[j, half, 0].astype(jnp.float32)
                + last_in[j, half].astype(jnp.float32)
            )
        ).astype(jnp.bfloat16)

    def both_halves(step, j):
        for half in range(HALVES):
            step(j, half)

    normalise(0)
    send_own(0)
    normalise(1)
    send_own(1)
    normalise(2)
    normalise(3)
    relay(0)
    send_own(2)
    relay(1)
    send_own(3)
    relay_last(0)
    compute(0)
    relay(2)
    relay_last(1)
    both_halves(first_hop, 0)
    compute(1)
    relay(3)
    relay_last(2)
    both_halves(first_hop, 1)
    both_halves(second_hop, 0)
    compute(2)
    relay_last(3)
    both_halves(first_hop, 2)
    both_halves(second_hop, 1)
    both_halves(finish, 0)
    compute(3)
    both_halves(first_hop, 3)
    both_halves(second_hop, 2)
    both_halves(finish, 1)
    both_halves(second_hop, 3)
    both_halves(finish, 2)
    both_halves(finish, 3)
    for copy in started:
        copy.wait_send()


def fused_block(*operands):
    queries, gates, gate_weight = operands[0], operands[4], operands[10]
    tokens, model_width = queries.shape
    devices = gates.shape[0]
    head_dim = model_width // devices
    hidden_width = gate_weight.shape[0]
    part = tokens // CHUNKS
    width = model_width // HALVES
    batch = devices * part
    near = pl.BlockSpec(memory_space=pltpu.VMEM)
    far = pl.BlockSpec(memory_space=pl.ANY)

    def space(*shape, kind=jnp.bfloat16):
        return pltpu.VMEM(shape, kind)

    def flags(*shape):
        return [pltpu.SemaphoreType.DMA(shape)] * 2

    return pl.pallas_call(
        fused_kernel,
        out_shape=jax.ShapeDtypeStruct((tokens, model_width), jnp.bfloat16),
        in_specs=[far] * 4 + [near] * 6 + [far] * 3,
        out_specs=near,
        scratch_shapes=[
            space(devices, 24, tokens, kind=jnp.float32),
            space(2 * devices, tokens, kind=jnp.float32),
            space(1, devices * tokens, kind=jnp.float32),
            space(CHUNKS, batch, 1, kind=jnp.float32),
            space(CHUNKS, batch, 1, kind=jnp.float32),
            space(CHUNKS, batch, head_dim),
            space(devices * tokens, head_dim),
            space(devices * tokens, head_dim),
            space(CHUNKS, batch, head_dim),
            space(CHUNKS, part, model_width),
            space(tokens, model_width),
            space(tokens, model_width),
            space(CHUNKS, batch, model_width),
            space(*gate_weight.shape),
            space(*gate_weight.shape),
            space(*gate_weight.shape),
            space(batch, hidden_width, kind=jnp.float32),
            space(batch, hidden_width, kind=jnp.float32),
            space(batch, hidden_width),
            space(2, HALVES, batch // 2, width),
            space(CHUNKS, HALVES, batch // 2, width),
            space(CHUNKS, HALVES, batch // 2, width),
            space(CHUNKS, HALVES, 2, part, width),
            space(CHUNKS, HALVES, 2, part, width),
            space(CHUNKS, HALVES, 2, part, width, kind=jnp.float32),
            space(CHUNKS, HALVES, part, width),
            space(CHUNKS, HALVES, part, width),
            pltpu.SemaphoreType.DMA((6 + CHUNKS,)),
        ]
        + flags(devices - 1)
        + flags(devices - 1)
        + flags(devices - 1)
        + flags(CHUNKS, devices - 1)
        + flags(CHUNKS, devices - 1)
        + flags(CHUNKS, 10)
        + flags(CHUNKS, HALVES)
        + flags(CHUNKS, HALVES, 2)
        + flags(CHUNKS, HALVES),
        compiler_params=pltpu.CompilerParams(
            collective_id=1, has_side_effects=True, vmem_limit_bytes=VMEM_BYTES
        ),
    )(*operands)


def shards(
    queries,
    key_vectors,
    value_vectors,
    residual_in,
    input_logit,
    forget_logit,
    mix_gain,
    ffn_gain,
    expert_gate,
    expert_up,
    expert_down,
    routes,
    route_weight,
):
    tokens, model_width = queries.shape
    head_count = input_logit.shape[0]
    head_dim = model_width // head_count
    devices = lax.axis_size("seq")
    group = devices // head_count
    group_width = model_width // devices
    if devices == 8 and head_count == 8:
        return fused_block(
            queries,
            key_vectors,
            value_vectors,
            residual_in,
            input_logit,
            forget_logit,
            jnp.transpose(routes),
            jnp.transpose(route_weight),
            mix_gain.reshape(1, -1),
            ffn_gain.reshape(1, -1),
            jnp.transpose(expert_gate[0]),
            jnp.transpose(expert_up[0]),
            expert_down[0],
        )

    capacity = 4 * tokens // devices
    flat_routes = routes.reshape(-1)
    matches = (flat_routes[:, None] == jnp.arange(devices, dtype=jnp.int32)[None, :]).astype(
        jnp.int32
    )
    before = jnp.cumsum(matches, axis=0) - matches
    position = jnp.sum(before * matches, axis=1)
    position = position.reshape(tokens, 2)
    slot_index = (flat_routes * capacity + position.reshape(-1)).reshape(tokens, 2)
    notes = jnp.stack(
        (jnp.repeat(input_logit, group, axis=0), jnp.repeat(forget_logit, group, axis=0)), axis=1
    )
    def columns_of(width, share):
        return lambda ref, other: ref.at[
            :, pl.ds(pl.multiple_of((other // share) * width, width), width)
        ]

    def rows_from(ref, origin):
        return ref.at[pl.ds(pl.multiple_of(origin * tokens, tokens), tokens), :]

    def entry(ref, other):
        return ref.at[other]

    head_columns = columns_of(head_dim, group)
    own_columns = columns_of(group_width, 1)
    tall = devices * tokens
    told, key_all, query_all, value_all = exchange(
        (
            (entry, entry),
            (head_columns, rows_from),
            (head_columns, rows_from),
            (own_columns, rows_from),
        ),
        devices,
        2,
        (notes, key_vectors, queries, value_vectors),
        (
            jax.ShapeDtypeStruct(notes.shape, jnp.float32),
            jax.ShapeDtypeStruct((tall, head_dim), jnp.bfloat16),
            jax.ShapeDtypeStruct((tall, head_dim), jnp.bfloat16),
            jax.ShapeDtypeStruct((tall, group_width), jnp.bfloat16),
        ),
    )
    mixed = head_mix(
        query_all, key_all, value_all, told[:, 0].reshape(-1), told[:, 1].reshape(-1)
    ).astype(jnp.bfloat16)
    (mixer_out,) = exchange(
        ((rows_from, own_columns),),
        devices,
        3,
        (mixed,),
        (jax.ShapeDtypeStruct((tokens, model_width), jnp.bfloat16),),
    )
    mixer_out = mixer_out.astype(jnp.float32)
    mixer_square = jnp.mean(mixer_out * mixer_out, axis=1, keepdims=True)
    updated = (
        residual_in.astype(jnp.float32) + mixer_out * lax.rsqrt(mixer_square + EPSILON) * mix_gain
    ).astype(jnp.bfloat16)
    updated_float = updated.astype(jnp.float32)
    updated_square = jnp.mean(updated_float * updated_float, axis=1, keepdims=True)
    normed = (updated_float * lax.rsqrt(updated_square + EPSILON) * ffn_gain).astype(jnp.bfloat16)
    columns = jnp.arange(devices * capacity, dtype=jnp.int32)
    pick_first = (slot_index[:, 0:1] == columns[None, :]).astype(jnp.bfloat16)
    pick_second = (slot_index[:, 1:2] == columns[None, :]).astype(jnp.bfloat16)
    spread = jnp.einsum(
        "tc,td->cd", pick_first + pick_second, normed, preferred_element_type=jnp.float32
    ).astype(jnp.bfloat16)
    outbound = spread.reshape(devices, capacity, model_width)
    block_in = lax.all_to_all(outbound, "seq", split_axis=0, concat_axis=0, tiled=True)
    row_block = block_in.reshape(-1, model_width)
    gate_val = jnp.dot(row_block, expert_gate[0], preferred_element_type=jnp.float32)
    up_val = jnp.dot(row_block, expert_up[0], preferred_element_type=jnp.float32)
    hidden = (jax.nn.silu(gate_val) * up_val).astype(jnp.bfloat16)
    result = jnp.dot(hidden, expert_down[0], preferred_element_type=jnp.float32).astype(
        jnp.bfloat16
    )
    inbound = lax.all_to_all(
        result.reshape(block_in.shape), "seq", split_axis=0, concat_axis=0, tiled=True
    )
    flat_back = inbound.reshape(devices * capacity, model_width)
    first_out = jnp.dot(pick_first, flat_back, preferred_element_type=jnp.float32)
    second_out = jnp.dot(pick_second, flat_back, preferred_element_type=jnp.float32)
    expert_mix = route_weight[:, 0:1] * first_out + route_weight[:, 1:2] * second_out
    return (updated_float + expert_mix).astype(jnp.bfloat16)


def solution(mesh):
    return jax.shard_map(
        shards,
        mesh=mesh,
        in_specs=(
            P(("batch", "seq"), None),
            P(("batch", "seq"), None),
            P(("batch", "seq"), None),
            P(("batch", "seq"), None),
            P(None, ("batch", "seq")),
            P(None, ("batch", "seq")),
            P(),
            P(),
            P("seq", None, None),
            P("seq", None, None),
            P("seq", None, None),
            P(("batch", "seq"), None),
            P(("batch", "seq"), None),
        ),
        out_specs=P(("batch", "seq"), None),
        check_vma=False,
    )
```

```python
import functools
import math

import jax
import jax.numpy as jnp
from jax import lax
from jax.experimental import pallas as pl
from jax.experimental.pallas import tpu as pltpu
from jax.sharding import PartitionSpec as P

EPSILON = 1e-06
CHUNKS = 4
HALVES = 2
FLIPS = (6, 4, 2, 7, 5, 3, 1)
SLOT_ORDER = (0, 2, 4, 6, 1, 3, 5, 7)
VMEM_BYTES = 64 * 1024 * 1024 - 2 * 1024 * 1024
LOW = -1e30


def exchange_kernel(moves, devices, *refs):
    count = len(moves)
    sources, targets = refs[:count], refs[count : 2 * count]
    send_sem, recv_sem, local_sem = refs[2 * count :]
    me = lax.axis_index("seq")
    others = [lax.rem(me + step, devices) for step in range(1, devices)]
    barrier = pltpu.get_barrier_semaphore()
    for other in others:
        pl.semaphore_signal(
            barrier, inc=1, device_id={"seq": other}, device_id_type=pl.DeviceIdType.MESH
        )
    pl.semaphore_wait(barrier, devices - 1)
    copies = []
    for i, (take, put) in enumerate(moves):
        for step, other in enumerate(others):
            copies.append(
                pltpu.make_async_remote_copy(
                    src_ref=take(sources[i], other),
                    dst_ref=put(targets[i], me),
                    send_sem=send_sem.at[i, step],
                    recv_sem=recv_sem.at[i, step],
                    device_id={"seq": other},
                    device_id_type=pl.DeviceIdType.MESH,
                )
            )
            copies[-1].start()
    for i, (take, put) in enumerate(moves):
        copies.append(
            pltpu.make_async_copy(take(sources[i], me), put(targets[i], me), local_sem.at[i])
        )
        copies[-1].start()
    for copy in copies:
        copy.wait()


def exchange(moves, devices, number, sources, shapes):
    far = pl.BlockSpec(memory_space=pl.ANY)
    count = len(moves)
    return pl.pallas_call(
        functools.partial(exchange_kernel, moves, devices),
        out_shape=shapes,
        in_specs=[far] * count,
        out_specs=[far] * count,
        scratch_shapes=[
            pltpu.SemaphoreType.DMA((count, devices - 1)),
            pltpu.SemaphoreType.DMA((count, devices - 1)),
            pltpu.SemaphoreType.DMA((count,)),
        ],
        compiler_params=pltpu.CompilerParams(collective_id=number, has_side_effects=True),
    )(*sources)


def head_mix(query, key, value, input_gate, forget_gate):
    positions, head_dim = query.shape
    cumul_log = jnp.cumsum(jax.nn.log_sigmoid(forget_gate))
    level = input_gate - cumul_log
    top = lax.cummax(level, axis=0)
    scores = lax.dot_general(
        query, key, (((1,), (1,)), ((), ())), preferred_element_type=jnp.float32
    )
    causal = jnp.arange(positions)[:, None] >= jnp.arange(positions)[None, :]
    decay = jnp.exp(jnp.minimum(level[None, :] - top[:, None], 0.0))
    coef = jnp.where(causal, decay * scores, 0.0) * (1.0 / math.sqrt(head_dim))
    denom_sum = jnp.sum(coef, axis=1, keepdims=True)
    numer_sum = jnp.dot(coef.astype(jnp.bfloat16), value, preferred_element_type=jnp.float32)
    return numer_sum / jnp.maximum(jnp.abs(denom_sum), 1.0)


def fused_kernel(
    query_far,
    key_far,
    value_far,
    residual_far,
    input_far,
    forget_far,
    routes_far,
    weights_far,
    mix_far,
    ffn_far,
    gate_far,
    up_far,
    down_far,
    out,
    input_gate,
    forget_gate,
    routes,
    weights,
    mix_gain,
    ffn_gain,
    info,
    gates,
    level,
    top,
    slot_weight,
    query_all,
    key_all,
    value_all,
    mixed,
    mixer_in,
    residual,
    updated,
    rows,
    gate,
    up,
    down,
    gate_sum,
    up_sum,
    hidden,
    own,
    core_out,
    core_in,
    hop_out,
    hop_in,
    keep,
    last_out,
    last_in,
    load_sem,
    info_send,
    info_recv,
    key_send,
    key_recv,
    value_send,
    value_recv,
    query_send,
    query_recv,
    mixed_send,
    mixed_recv,
    gather_send,
    gather_recv,
    core_send,
    core_recv,
    hop_send,
    hop_recv,
    last_send,
    last_recv,
):
    me = lax.axis_index("seq")
    heads, tokens = input_gate.shape
    devices = heads
    head_dim = key_all.shape[1]
    part = tokens // CHUNKS
    width = out.shape[1] // HALVES
    four = devices // 2 * part

    def peer(flip):
        total = 0
        for bit in (1, 2, 4):
            own_bit = lax.rem(lax.div(me, bit), 2)
            total = total + bit * ((1 - own_bit) if flip & bit else own_bit)
        return total

    def arrive(whole, flag):
        pltpu.make_async_copy(whole, whole, flag).wait()

    def remote(source, target, send_sem, recv_sem, flip):
        copy = pltpu.make_async_remote_copy(
            src_ref=source,
            dst_ref=target,
            send_sem=send_sem,
            recv_sem=recv_sem,
            device_id={"seq": peer(flip)},
            device_id_type=pl.DeviceIdType.MESH,
        )
        copy.start()
        return copy

    def block_rows(origin, count):
        return pl.ds(pl.multiple_of(origin * count, count), count)

    def head_columns(origin):
        return pl.ds(pl.multiple_of(origin * head_dim, head_dim), head_dim)

    barrier = pltpu.get_barrier_semaphore()
    for flip in FLIPS:
        pl.semaphore_signal(
            barrier,
            inc=1,
            device_id={"seq": peer(flip)},
            device_id_type=pl.DeviceIdType.MESH,
        )
    loads = [
        pltpu.make_async_copy(source, target, load_sem.at[i])
        for i, (source, target) in enumerate(
            (
                (key_far.at[:, head_columns(me)], key_all.at[block_rows(me, tokens), :]),
                (value_far.at[:, head_columns(me)], value_all.at[block_rows(me, tokens), :]),
                (residual_far, residual),
                (gate_far, gate),
                (up_far, up),
                (down_far, down),
            )
            + tuple(
                (
                    query_far.at[pl.ds(j * part, part), head_columns(me)],
                    query_all.at[j, block_rows(me, part), :],
                )
                for j in range(CHUNKS)
            )
            + (
                (input_far, input_gate),
                (forget_far, forget_gate),
                (routes_far, routes),
                (weights_far, weights),
                (mix_far, mix_gain),
                (ffn_far, ffn_gain),
            )
        )
    ]
    for load in loads[-6:] + loads[:3] + loads[6:-6]:
        load.start()
    for load in loads[-6:]:
        load.wait()
    forget = forget_gate[...]
    info[me, 0:8, :] = input_gate[...]
    info[me, 8:16, :] = -(jnp.maximum(-forget, 0.0) + jnp.log1p(jnp.exp(-jnp.abs(forget))))
    info[me, 16:18, :] = routes[...].astype(jnp.float32)
    info[me, 18:20, :] = weights[...]
    pl.semaphore_wait(barrier, devices - 1)

    for flip in FLIPS:
        remote(
            key_far.at[:, head_columns(peer(flip))],
            key_all.at[block_rows(me, tokens), :],
            key_send.at[0],
            key_recv.at[0],
            flip,
        )
        remote(
            info.at[me], info.at[me], info_send.at[0], info_recv.at[0], flip
        )
    for flip in FLIPS:
        remote(
            value_far.at[:, head_columns(peer(flip))],
            value_all.at[block_rows(me, tokens), :],
            value_send.at[0],
            value_recv.at[0],
            flip,
        )
    for j in range(CHUNKS):
        for flip in FLIPS:
            remote(
                query_far.at[pl.ds(j * part, part), head_columns(peer(flip))],
                query_all.at[j, block_rows(me, part), :],
                query_send.at[0],
                query_recv.at[j],
                flip,
            )
    for load in loads[3:6]:
        load.start()

    arrive(info.at[1:], info_recv.at[0])
    for block in range(devices):
        gates[block : block + 1, :] = info[block, pl.ds(me, 1), :]
        gates[devices + block : devices + block + 1, :] = info[block, pl.ds(heads + me, 1), :]
    across = lax.broadcasted_iota(jnp.int32, (tokens, tokens), 0)
    along = lax.broadcasted_iota(jnp.int32, (tokens, tokens), 1)
    local_sum = jnp.dot(
        gates[devices : 2 * devices, :],
        (across <= along).astype(jnp.float32),
        precision=lax.Precision.HIGHEST,
        preferred_element_type=jnp.float32,
    )
    before = jnp.zeros((1, 1), jnp.float32)
    peak = jnp.full((1, 1), LOW, jnp.float32)
    for block in range(devices):
        line = local_sum[block : block + 1, :]
        level_line = gates[block : block + 1, :] - (line + before)
        before = before + line[:, tokens - 1 : tokens]
        level[:, block * tokens : (block + 1) * tokens] = level_line
        spread = jnp.where(along <= across, jnp.broadcast_to(level_line, (tokens, tokens)), LOW)
        tops = jnp.maximum(jnp.max(spread, axis=1, keepdims=True), peak)
        peak = jnp.maximum(peak, jnp.max(level_line, axis=1, keepdims=True))
        for j in range(CHUNKS):
            top[j, block * part : (block + 1) * part, :] = tops[j * part : (j + 1) * part, :]
    for slot in range(devices):
        told = info.at[peer(slot)] if slot else info.at[me]
        line = jnp.where(told[16:17, :].astype(jnp.int32) == me, told[18:19, :], 0.0) + jnp.where(
            told[17:18, :].astype(jnp.int32) == me, told[19:20, :], 0.0
        )
        spread = jnp.where(along == across, jnp.broadcast_to(line, (tokens, tokens)), 0.0)
        column = jnp.sum(spread, axis=1, keepdims=True)
        place = SLOT_ORDER.index(slot) * part
        for j in range(CHUNKS):
            slot_weight[j, place : place + part, :] = column[j * part : (j + 1) * part, :]

    arrive(key_all.at[tokens:, :], key_recv.at[0])
    arrive(value_all.at[tokens:, :], value_recv.at[0])
    loads[0].wait()
    loads[1].wait()
    place_in = lax.broadcasted_iota(jnp.int32, (devices * part, 1), 0)
    place_in = lax.shift_right_logical(place_in, part.bit_length() - 1) * (tokens - part) + place_in
    place_key = lax.broadcasted_iota(jnp.int32, (1, devices * tokens), 1)
    for j in range(CHUNKS):
        arrive(query_all.at[j, part:, :], query_recv.at[j])
        loads[6 + j].wait()
        scores = lax.dot_general(
            query_all[j],
            key_all[...],
            (((1,), (1,)), ((), ())),
            preferred_element_type=jnp.float32,
        )
        decay = jnp.exp(jnp.minimum(level[...] - top[j], 0.0))
        coef = jnp.where(place_key <= place_in + j * part, decay * scores, 0.0) * (
            1.0 / math.sqrt(head_dim)
        )
        denom_sum = jnp.sum(coef, axis=1, keepdims=True)
        numer_sum = jnp.dot(
            coef.astype(jnp.bfloat16), value_all[...], preferred_element_type=jnp.float32
        )
        mixed[j] = (numer_sum / jnp.maximum(jnp.abs(denom_sum), 1.0)).astype(jnp.bfloat16)
        for flip in FLIPS:
            remote(
                mixed.at[j, block_rows(peer(flip), part), :],
                mixer_in.at[j, :, head_columns(me)],
                mixed_send.at[0],
                mixed_recv.at[j],
                flip,
            )
        mixer_in[j, :, head_columns(me)] = mixed[j, block_rows(me, part), :]

    def slot_rows(slot):
        return pl.ds(SLOT_ORDER.index(slot) * part, part)

    def columns(half):
        return pl.ds(half * width, width)

    gathers = {}

    def gather(j, number, source, target, flip, half=None):
        view = slice(None) if half is None else columns(half)
        gathers[j, number] = remote(
            rows.at[j, slot_rows(source), view],
            rows.at[j, slot_rows(target), view],
            gather_send.at[0],
            gather_recv.at[j, number],
            flip,
        )

    def normalise(j):
        arrive(mixer_in.at[j, :, head_dim:], mixed_recv.at[j])
        if j == 0:
            loads[2].wait()
        span = slice(j * part, (j + 1) * part)
        mixer_out = mixer_in[j].astype(jnp.float32)
        square = jnp.mean(mixer_out * mixer_out, axis=1, keepdims=True)
        value = (
            residual[span, :].astype(jnp.float32)
            + mixer_out * lax.rsqrt(square + EPSILON) * mix_gain[...]
        ).astype(jnp.bfloat16)
        updated[span, :] = value
        value = value.astype(jnp.float32)
        square = jnp.mean(value * value, axis=1, keepdims=True)
        rows[j, 0:part, :] = (value * lax.rsqrt(square + EPSILON) * ffn_gain[...]).astype(
            jnp.bfloat16
        )

    def send_own(j):
        gather(j, 0, 0, 2, 2, 0)
        gather(j, 1, 0, 4, 4, 1)
        gather(j, 2, 0, 2, 2, 1)
        gather(j, 3, 0, 4, 4, 0)
        gather(j, 4, 0, 1, 1)

    def relay(j):
        gathers[j, 0].wait_recv()
        gather(j, 5, 2, 6, 4, 0)
        gathers[j, 1].wait_recv()
        gather(j, 6, 4, 6, 2, 1)
        gathers[j, 2].wait_recv()
        gather(j, 7, 2, 3, 1)
        gathers[j, 3].wait_recv()
        gather(j, 8, 4, 5, 1)

    def relay_last(j):
        gathers[j, 5].wait_recv()
        gathers[j, 6].wait_recv()
        gather(j, 9, 6, 7, 1)

    core_copies, hop_copies, last_copies = {}, {}, {}

    def compute(j):
        for number in (4, 7, 8, 9):
            gathers[j, number].wait_recv()
        if j == 0:
            loads[3].wait()
            loads[4].wait()
        for weight, total in ((gate, gate_sum), (up, up_sum)):
            total[...] = lax.dot_general(
                rows[j],
                weight[...],
                (((1,), (1,)), ((), ())),
                preferred_element_type=jnp.float32,
            )
        gate_val = gate_sum[...]
        hidden[...] = (gate_val / (1.0 + jnp.exp(-gate_val)) * up_sum[...]).astype(jnp.bfloat16)
        if j == 0:
            loads[5].wait()
        for half in range(HALVES):
            terms = (
                jnp.dot(hidden[...], down[:, columns(half)], preferred_element_type=jnp.float32)
                * slot_weight[j]
            ).astype(jnp.bfloat16)
            own[j % 2, half] = terms[:four, :]
            core_out[j, half] = terms[four:, :]
            core_copies[j, half] = remote(
                core_out.at[j, half],
                core_in.at[j, half],
                core_send.at[0],
                core_recv.at[j, half],
                1,
            )

    def first_hop(j, half):
        first, second = (2, 4) if half == 0 else (4, 2)
        core_copies[j, half].wait_recv()
        for slot in (6, first, second, 0):
            view = slot_rows(slot)
            both = own[j % 2, half, view, :].astype(jnp.float32) + core_in[
                j, half, view, :
            ].astype(jnp.float32)
            if slot in (0, second):
                keep[j, half, 0 if slot == 0 else 1] = both
                continue
            place = 1 if slot == 6 else 0
            hop_out[j, half, place] = both.astype(jnp.bfloat16)
            hop_copies[j, half, place] = remote(
                hop_out.at[j, half, place],
                hop_in.at[j, half, place],
                hop_send.at[0],
                hop_recv.at[j, half, place],
                first,
            )

    def second_hop(j, half):
        second = 4 if half == 0 else 2
        hop_copies[j, half, 1].wait_recv()
        last_out[j, half] = (
            keep[j, half, 1] + hop_in[j, half, 1].astype(jnp.float32)
        ).astype(jnp.bfloat16)
        last_copies[j, half] = remote(
            last_out.at[j, half],
            last_in.at[j, half],
            last_send.at[0],
            last_recv.at[j, half],
            second,
        )

    def finish(j, half):
        hop_copies[j, half, 0].wait_recv()
        last_copies[j, half].wait_recv()
        span = slice(j * part, (j + 1) * part)
        out[span, columns(half)] = (
            updated[span, columns(half)].astype(jnp.float32)
            + (
                keep[j, half, 0]
                + hop_in[j, half, 0].astype(jnp.float32)
                + last_in[j, half].astype(jnp.float32)
            )
        ).astype(jnp.bfloat16)

    def both_halves(step, j):
        for half in range(HALVES):
            step(j, half)

    normalise(0)
    send_own(0)
    normalise(1)
    send_own(1)
    normalise(2)
    normalise(3)
    relay(0)
    send_own(2)
    relay(1)
    send_own(3)
    relay_last(0)
    compute(0)
    relay(2)
    relay_last(1)
    both_halves(first_hop, 0)
    compute(1)
    relay(3)
    relay_last(2)
    both_halves(first_hop, 1)
    both_halves(second_hop, 0)
    compute(2)
    relay_last(3)
    both_halves(first_hop, 2)
    both_halves(second_hop, 1)
    both_halves(finish, 0)
    compute(3)
    both_halves(first_hop, 3)
    both_halves(second_hop, 2)
    both_halves(finish, 1)
    both_halves(second_hop, 3)
    both_halves(finish, 2)
    both_halves(finish, 3)
    for whole, flag in (
        (info.at[1:], info_send),
        (key_all.at[tokens:, :], key_send),
        (value_all.at[tokens:, :], value_send),
        (query_all.at[:, part:, :], query_send),
        (mixed.at[:, part:, :], mixed_send),
        (rows.at[:, part:, :], gather_send),
        (core_out, core_send),
        (hop_out, hop_send),
        (last_out, last_send),
    ):
        arrive(whole, flag.at[0])


def fused_block(*operands):
    queries, gates, gate_weight = operands[0], operands[4], operands[10]
    tokens, model_width = queries.shape
    devices = gates.shape[0]
    head_dim = model_width // devices
    hidden_width = gate_weight.shape[0]
    part = tokens // CHUNKS
    width = model_width // HALVES
    batch = devices * part
    near = pl.BlockSpec(memory_space=pltpu.VMEM)
    far = pl.BlockSpec(memory_space=pl.ANY)

    def space(*shape, kind=jnp.bfloat16):
        return pltpu.VMEM(shape, kind)

    def flags(*shape):
        return [pltpu.SemaphoreType.DMA((1,)), pltpu.SemaphoreType.DMA(shape)]

    return pl.pallas_call(
        fused_kernel,
        out_shape=pltpu.VMEM((tokens, model_width), jnp.bfloat16),
        in_specs=[far] * 13,
        out_specs=near,
        scratch_shapes=[
            space(devices, tokens, kind=jnp.float32),
            space(devices, tokens, kind=jnp.float32),
            space(2, tokens, kind=jnp.int32),
            space(2, tokens, kind=jnp.float32),
            space(1, model_width, kind=jnp.float32),
            space(1, model_width, kind=jnp.float32),
            space(devices, 24, tokens, kind=jnp.float32),
            space(2 * devices, tokens, kind=jnp.float32),
            space(1, devices * tokens, kind=jnp.float32),
            space(CHUNKS, batch, 1, kind=jnp.float32),
            space(CHUNKS, batch, 1, kind=jnp.float32),
            space(CHUNKS, batch, head_dim),
            space(devices * tokens, head_dim),
            space(devices * tokens, head_dim),
            space(CHUNKS, batch, head_dim),
            space(CHUNKS, part, model_width),
            space(tokens, model_width),
            space(tokens, model_width),
            space(CHUNKS, batch, model_width),
            space(*gate_weight.shape),
            space(*gate_weight.shape),
            space(*gate_weight.shape),
            space(batch, hidden_width, kind=jnp.float32),
            space(batch, hidden_width, kind=jnp.float32),
            space(batch, hidden_width),
            space(2, HALVES, batch // 2, width),
            space(CHUNKS, HALVES, batch // 2, width),
            space(CHUNKS, HALVES, batch // 2, width),
            space(CHUNKS, HALVES, 2, part, width),
            space(CHUNKS, HALVES, 2, part, width),
            space(CHUNKS, HALVES, 2, part, width, kind=jnp.float32),
            space(CHUNKS, HALVES, part, width),
            space(CHUNKS, HALVES, part, width),
            pltpu.SemaphoreType.DMA((12 + CHUNKS,)),
        ]
        + flags(1)
        + flags(1)
        + flags(1)
        + flags(CHUNKS)
        + flags(CHUNKS)
        + flags(CHUNKS, 10)
        + flags(CHUNKS, HALVES)
        + flags(CHUNKS, HALVES, 2)
        + flags(CHUNKS, HALVES),
        compiler_params=pltpu.CompilerParams(
            collective_id=1, has_side_effects=True, vmem_limit_bytes=VMEM_BYTES
        ),
    )(*operands)


def shards(
    queries,
    key_vectors,
    value_vectors,
    residual_in,
    input_logit,
    forget_logit,
    mix_gain,
    ffn_gain,
    expert_gate,
    expert_up,
    expert_down,
    routes,
    route_weight,
):
    tokens, model_width = queries.shape
    head_count = input_logit.shape[0]
    head_dim = model_width // head_count
    devices = lax.axis_size("seq")
    group = devices // head_count
    group_width = model_width // devices
    if devices == 8 and head_count == 8:
        return fused_block(
            queries,
            key_vectors,
            value_vectors,
            residual_in,
            input_logit,
            forget_logit,
            jnp.transpose(routes),
            jnp.transpose(route_weight),
            mix_gain.reshape(1, -1),
            ffn_gain.reshape(1, -1),
            jnp.transpose(expert_gate[0]),
            jnp.transpose(expert_up[0]),
            expert_down[0],
        )

    capacity = 4 * tokens // devices
    flat_routes = routes.reshape(-1)
    matches = (flat_routes[:, None] == jnp.arange(devices, dtype=jnp.int32)[None, :]).astype(
        jnp.int32
    )
    before = jnp.cumsum(matches, axis=0) - matches
    position = jnp.sum(before * matches, axis=1)
    position = position.reshape(tokens, 2)
    slot_index = (flat_routes * capacity + position.reshape(-1)).reshape(tokens, 2)
    notes = jnp.stack(
        (jnp.repeat(input_logit, group, axis=0), jnp.repeat(forget_logit, group, axis=0)), axis=1
    )
    def columns_of(width, share):
        return lambda ref, other: ref.at[
            :, pl.ds(pl.multiple_of((other // share) * width, width), width)
        ]

    def rows_from(ref, origin):
        return ref.at[pl.ds(pl.multiple_of(origin * tokens, tokens), tokens), :]

    def entry(ref, other):
        return ref.at[other]

    head_columns = columns_of(head_dim, group)
    own_columns = columns_of(group_width, 1)
    tall = devices * tokens
    told, key_all, query_all, value_all = exchange(
        (
            (entry, entry),
            (head_columns, rows_from),
            (head_columns, rows_from),
            (own_columns, rows_from),
        ),
        devices,
        2,
        (notes, key_vectors, queries, value_vectors),
        (
            jax.ShapeDtypeStruct(notes.shape, jnp.float32),
            jax.ShapeDtypeStruct((tall, head_dim), jnp.bfloat16),
            jax.ShapeDtypeStruct((tall, head_dim), jnp.bfloat16),
            jax.ShapeDtypeStruct((tall, group_width), jnp.bfloat16),
        ),
    )
    mixed = head_mix(
        query_all, key_all, value_all, told[:, 0].reshape(-1), told[:, 1].reshape(-1)
    ).astype(jnp.bfloat16)
    (mixer_out,) = exchange(
        ((rows_from, own_columns),),
        devices,
        3,
        (mixed,),
        (jax.ShapeDtypeStruct((tokens, model_width), jnp.bfloat16),),
    )
    mixer_out = mixer_out.astype(jnp.float32)
    mixer_square = jnp.mean(mixer_out * mixer_out, axis=1, keepdims=True)
    updated = (
        residual_in.astype(jnp.float32) + mixer_out * lax.rsqrt(mixer_square + EPSILON) * mix_gain
    ).astype(jnp.bfloat16)
    updated_float = updated.astype(jnp.float32)
    updated_square = jnp.mean(updated_float * updated_float, axis=1, keepdims=True)
    normed = (updated_float * lax.rsqrt(updated_square + EPSILON) * ffn_gain).astype(jnp.bfloat16)
    columns = jnp.arange(devices * capacity, dtype=jnp.int32)
    pick_first = (slot_index[:, 0:1] == columns[None, :]).astype(jnp.bfloat16)
    pick_second = (slot_index[:, 1:2] == columns[None, :]).astype(jnp.bfloat16)
    spread = jnp.einsum(
        "tc,td->cd", pick_first + pick_second, normed, preferred_element_type=jnp.float32
    ).astype(jnp.bfloat16)
    outbound = spread.reshape(devices, capacity, model_width)
    block_in = lax.all_to_all(outbound, "seq", split_axis=0, concat_axis=0, tiled=True)
    row_block = block_in.reshape(-1, model_width)
    gate_val = jnp.dot(row_block, expert_gate[0], preferred_element_type=jnp.float32)
    up_val = jnp.dot(row_block, expert_up[0], preferred_element_type=jnp.float32)
    hidden = (jax.nn.silu(gate_val) * up_val).astype(jnp.bfloat16)
    result = jnp.dot(hidden, expert_down[0], preferred_element_type=jnp.float32).astype(
        jnp.bfloat16
    )
    inbound = lax.all_to_all(
        result.reshape(block_in.shape), "seq", split_axis=0, concat_axis=0, tiled=True
    )
    flat_back = inbound.reshape(devices * capacity, model_width)
    first_out = jnp.dot(pick_first, flat_back, preferred_element_type=jnp.float32)
    second_out = jnp.dot(pick_second, flat_back, preferred_element_type=jnp.float32)
    expert_mix = route_weight[:, 0:1] * first_out + route_weight[:, 1:2] * second_out
    return (updated_float + expert_mix).astype(jnp.bfloat16)


def solution(mesh):
    return jax.shard_map(
        shards,
        mesh=mesh,
        in_specs=(
            P(("batch", "seq"), None),
            P(("batch", "seq"), None),
            P(("batch", "seq"), None),
            P(("batch", "seq"), None),
            P(None, ("batch", "seq")),
            P(None, ("batch", "seq")),
            P(),
            P(),
            P("seq", None, None),
            P("seq", None, None),
            P("seq", None, None),
            P(("batch", "seq"), None),
            P(("batch", "seq"), None),
        ),
        out_specs=P(("batch", "seq"), None),
        check_vma=False,
    )
```

```python
import functools
import math

import jax
import jax.numpy as jnp
from jax import lax
from jax.experimental import pallas as pl
from jax.experimental.pallas import tpu as pltpu
from jax.sharding import PartitionSpec as P

EPSILON = 1e-06
CHUNKS = 4
HALVES = 2
FLIPS = (6, 4, 2, 7, 5, 3, 1)
SLOT_ORDER = (0, 2, 4, 6, 1, 3, 5, 7)
VMEM_BYTES = 64 * 1024 * 1024 - 1280 * 1024
LOW = -1e30


def exchange_kernel(moves, devices, *refs):
    count = len(moves)
    sources, targets = refs[:count], refs[count : 2 * count]
    send_sem, recv_sem, local_sem = refs[2 * count :]
    me = lax.axis_index("seq")
    others = [lax.rem(me + step, devices) for step in range(1, devices)]
    barrier = pltpu.get_barrier_semaphore()
    for other in others:
        pl.semaphore_signal(
            barrier, inc=1, device_id={"seq": other}, device_id_type=pl.DeviceIdType.MESH
        )
    pl.semaphore_wait(barrier, devices - 1)
    copies = []
    for i, (take, put) in enumerate(moves):
        for step, other in enumerate(others):
            copies.append(
                pltpu.make_async_remote_copy(
                    src_ref=take(sources[i], other),
                    dst_ref=put(targets[i], me),
                    send_sem=send_sem.at[i, step],
                    recv_sem=recv_sem.at[i, step],
                    device_id={"seq": other},
                    device_id_type=pl.DeviceIdType.MESH,
                )
            )
            copies[-1].start()
    for i, (take, put) in enumerate(moves):
        copies.append(
            pltpu.make_async_copy(take(sources[i], me), put(targets[i], me), local_sem.at[i])
        )
        copies[-1].start()
    for copy in copies:
        copy.wait()


def exchange(moves, devices, number, sources, shapes):
    far = pl.BlockSpec(memory_space=pl.ANY)
    count = len(moves)
    return pl.pallas_call(
        functools.partial(exchange_kernel, moves, devices),
        out_shape=shapes,
        in_specs=[far] * count,
        out_specs=[far] * count,
        scratch_shapes=[
            pltpu.SemaphoreType.DMA((count, devices - 1)),
            pltpu.SemaphoreType.DMA((count, devices - 1)),
            pltpu.SemaphoreType.DMA((count,)),
        ],
        compiler_params=pltpu.CompilerParams(collective_id=number, has_side_effects=True),
    )(*sources)


def head_mix(query, key, value, input_gate, forget_gate):
    positions, head_dim = query.shape
    cumul_log = jnp.cumsum(jax.nn.log_sigmoid(forget_gate))
    level = input_gate - cumul_log
    top = lax.cummax(level, axis=0)
    scores = lax.dot_general(
        query, key, (((1,), (1,)), ((), ())), preferred_element_type=jnp.float32
    )
    causal = jnp.arange(positions)[:, None] >= jnp.arange(positions)[None, :]
    decay = jnp.exp(jnp.minimum(level[None, :] - top[:, None], 0.0))
    coef = jnp.where(causal, decay * scores, 0.0) * (1.0 / math.sqrt(head_dim))
    denom_sum = jnp.sum(coef, axis=1, keepdims=True)
    numer_sum = jnp.dot(coef.astype(jnp.bfloat16), value, preferred_element_type=jnp.float32)
    return numer_sum / jnp.maximum(jnp.abs(denom_sum), 1.0)


def fused_kernel(
    query_far,
    key_far,
    value_far,
    residual_far,
    input_far,
    forget_far,
    routes_far,
    weights_far,
    mix_far,
    ffn_far,
    gate_far,
    up_far,
    down_far,
    out,
    input_gate,
    forget_gate,
    routes,
    weights,
    mix_gain,
    ffn_gain,
    info,
    level,
    peak_before,
    key_level,
    top,
    slot_weight,
    query_wide,
    query_slim,
    key_wide,
    value_wide,
    key_slim,
    value_slim,
    reply_wide,
    reply_slim,
    from_far_row,
    from_near_wide,
    from_near_slim,
    denom,
    mixed,
    mixer_in,
    updated,
    rows,
    gate,
    up,
    down,
    gate_sum,
    up_sum,
    hidden,
    own,
    core_out,
    core_in,
    hop_out,
    hop_in,
    keep,
    last_out,
    last_in,
    load_sem,
    info_sem,
    pair_send,
    pair_recv,
    far_sem,
    wide_send,
    wide_recv,
    slim_send,
    slim_recv,
    reply_send,
    reply_recv,
    mixed_send,
    mixed_recv,
    gather_send,
    gather_recv,
    core_send,
    core_recv,
    hop_send,
    hop_recv,
    last_send,
    last_recv,
):
    me = lax.axis_index("seq")
    heads, tokens = input_gate.shape
    devices = heads
    model_width = out.shape[1]
    head_dim = model_width // heads
    part = tokens // CHUNKS
    width = model_width // HALVES
    four = devices // 2 * part
    slice_width = 2 * head_dim
    core = lax.rem(me, 2)
    column = lax.rem(lax.div(me, 2), 2)
    row = lax.div(me, 4)
    chip = lax.div(me, 2)
    chip_x = chip + 1 - 2 * column
    chip_y = chip + 2 - 4 * row
    key_chip = chip_x * (1 - row) + chip_y * row
    query_chip = chip_y * (1 - row) + chip_x * row
    wide_base = (1 - row) * width
    slim_base = row * width
    bases = (wide_base, slim_base)

    def peer(flip):
        total = 0
        for bit in (1, 2, 4):
            own_bit = lax.rem(lax.div(me, bit), 2)
            total = total + bit * ((1 - own_bit) if flip & bit else own_bit)
        return total

    def arrive(whole, flag):
        pltpu.make_async_copy(whole, whole, flag).wait()

    def prepared(source, target, send_sem, recv_sem, flip):
        return pltpu.make_async_remote_copy(
            src_ref=source,
            dst_ref=target,
            send_sem=send_sem,
            recv_sem=recv_sem,
            device_id={"seq": peer(flip)},
            device_id_type=pl.DeviceIdType.MESH,
        )

    def remote(*arguments):
        copy = prepared(*arguments)
        copy.start()
        return copy

    def span_of(index, count, first=0):
        return pl.ds(pl.multiple_of(index * count + first, count), count)

    def head_columns(base, owner):
        return pl.ds(pl.multiple_of(base + owner * slice_width, slice_width), slice_width)

    def core_of(flip):
        return 1 - core if flip % 2 else core

    barrier = pltpu.get_barrier_semaphore()
    for flip in FLIPS:
        pl.semaphore_signal(
            barrier,
            inc=1,
            device_id={"seq": peer(flip)},
            device_id_type=pl.DeviceIdType.MESH,
        )
    small = (
        (input_far, input_gate),
        (forget_far, forget_gate),
        (routes_far, routes),
        (weights_far, weights),
        (mix_far, mix_gain),
        (ffn_far, ffn_gain),
    )
    blocks = tuple(
        (far.at[:, head_columns(base, core)], target.at[span_of(core, tokens), :])
        for base, far, target in (
            (wide_base, key_far, key_wide),
            (wide_base, value_far, value_wide),
            (slim_base, key_far, key_slim),
            (slim_base, value_far, value_slim),
        )
    ) + tuple(
        (
            query_far.at[pl.ds(j * part, part), head_columns(base, core)],
            target.at[j, span_of(core, part), :],
        )
        for j in range(CHUNKS)
        for base, target in ((wide_base, query_wide), (slim_base, query_slim))
    )
    large = ((residual_far, updated), (gate_far, gate), (up_far, up), (down_far, down))
    loads = [
        pltpu.make_async_copy(source, target, load_sem.at[i])
        for i, (source, target) in enumerate(small + blocks + large)
    ]
    small_loads, block_loads, large_loads = loads[:6], loads[6:18], loads[18:]
    for load in small_loads + block_loads:
        load.start()
    for load in small_loads:
        load.wait()
    forget = forget_gate[...]
    info[me, 0:8, :] = input_gate[...]
    info[me, 8:16, :] = -(jnp.maximum(-forget, 0.0) + jnp.log1p(jnp.exp(-jnp.abs(forget))))
    info[me, 16:18, :] = routes[...].astype(jnp.float32)
    info[me, 18:20, :] = weights[...]
    pl.semaphore_wait(barrier, devices - 1)

    for flip in FLIPS:
        remote(info.at[me], info.at[me], info_sem.at[0], info_sem.at[1], flip)

    @pl.when(row == 0)
    def send_keys():
        for far, target in ((key_far, key_wide), (value_far, value_wide)):
            for flip, base in ((2, wide_base), (4, slim_base), (3, wide_base), (5, slim_base)):
                remote(
                    far.at[:, head_columns(base, core_of(flip))],
                    target.at[span_of(core, tokens, 2 * tokens), :],
                    far_sem.at[0],
                    far_sem.at[1],
                    flip,
                )

    @pl.when(column == 1)
    def send_slim_queries():
        for j in range(CHUNKS):
            for flip in (2, 3):
                remote(
                    query_far.at[pl.ds(j * part, part), head_columns(slim_base, core_of(flip))],
                    query_slim.at[j, span_of(core, part, 2 * part), :],
                    slim_send.at[0],
                    slim_recv.at[j],
                    flip,
                )

    @pl.when(row == 1)
    def send_wide_queries():
        for j in range(CHUNKS):
            for flip, base in ((2, wide_base), (4, slim_base), (3, wide_base), (5, slim_base)):
                remote(
                    query_far.at[pl.ds(j * part, part), head_columns(base, core_of(flip))],
                    query_wide.at[j, span_of(core, part, 2 * part), :],
                    wide_send.at[0],
                    wide_recv.at[j],
                    flip,
                )

    for base, far, target in (
        (wide_base, key_far, key_wide),
        (wide_base, value_far, value_wide),
        (slim_base, key_far, key_slim),
        (slim_base, value_far, value_slim),
    ):
        remote(
            far.at[:, head_columns(base, 1 - core)],
            target.at[span_of(core, tokens), :],
            pair_send.at[0],
            pair_recv.at[CHUNKS],
            1,
        )
    for j in range(CHUNKS):
        for base, target in ((wide_base, query_wide), (slim_base, query_slim)):
            remote(
                query_far.at[pl.ds(j * part, part), head_columns(base, 1 - core)],
                target.at[j, span_of(core, part), :],
                pair_send.at[1],
                pair_recv.at[j],
                1,
            )
    for load in large_loads:
        load.start()

    arrive(info.at[1:], info_sem.at[1])
    across = lax.broadcasted_iota(jnp.int32, (tokens, tokens), 0)
    along = lax.broadcasted_iota(jnp.int32, (tokens, tokens), 1)
    local_sum = jnp.dot(
        info[:, 8:16, :].reshape(devices * heads, tokens),
        (across <= along).astype(jnp.float32),
        precision=lax.Precision.HIGHEST,
        preferred_element_type=jnp.float32,
    )
    before = jnp.zeros((heads, 1), jnp.float32)
    peak = jnp.full((heads, 1), LOW, jnp.float32)
    for block in range(devices):
        lines = local_sum[block * heads : (block + 1) * heads, :]
        level_lines = info[block, 0:8, :] - (lines + before)
        before = before + lines[:, tokens - 1 : tokens]
        level[block] = level_lines
        peak_before[block] = jnp.broadcast_to(peak, (heads, tokens))
        peak = jnp.maximum(peak, jnp.max(level_lines, axis=1, keepdims=True))
    for group, first_chip in ((0, query_chip), (1, chip_x)):
        for i in range(2):
            head = (row if group else 1 - row) * (heads // 2) + 2 * core + i
            for slot in range(4):
                block = 2 * (chip if slot < 2 else first_chip) + slot % 2
                line = level[block, pl.ds(head, 1), :]
                if slot < 2:
                    key_level[2 * group + i, :, slot * tokens : (slot + 1) * tokens] = line
                spread = jnp.where(along <= across, jnp.broadcast_to(line, (tokens, tokens)), LOW)
                tops = jnp.maximum(
                    jnp.max(spread, axis=1, keepdims=True),
                    peak_before[block, pl.ds(head, 1), :][:, 0:1],
                )
                for j in range(CHUNKS):
                    top[j, slot * part : (slot + 1) * part, 2 * group + i : 2 * group + i + 1] = (
                        tops[j * part : (j + 1) * part, :]
                    )
            if group == 0:
                for slot in (2, 3):
                    key_level[i, :, slot * tokens : (slot + 1) * tokens] = level[
                        2 * key_chip + slot % 2, pl.ds(head, 1), :
                    ]

    query_row = lax.broadcasted_iota(jnp.int32, (4 * part, 1), 0)
    row_block = lax.shift_right_logical(query_row, part.bit_length() - 1)
    foreign_row = row_block >= 2
    row_place = (
        jnp.where(foreign_row, row_block - 2, row_block) * (tokens - part)
        + query_row
        - jnp.where(foreign_row, 2 * part, 0)
    )
    lane = lax.broadcasted_iota(jnp.int32, (2 * part, tokens), 1)
    key_lane = lax.broadcasted_iota(jnp.int32, (1, 4 * tokens), 1)
    wide_place = jnp.where(
        key_lane < 2 * tokens,
        chip * (2 * tokens) + key_lane,
        key_chip * (2 * tokens) + key_lane - 2 * tokens,
    )

    def attend(j, group, query, key, value, key_place, foreign_chip, reply):
        place = row_place + j * part + jnp.where(foreign_row, foreign_chip, chip) * (2 * tokens)
        causal = key_place <= place
        keys = key.shape[0]
        extra = jnp.zeros((2 * part, tokens), jnp.float32)
        for i in range(2):
            number = 2 * group + i
            view = slice(i * head_dim, (i + 1) * head_dim)
            scores = lax.dot_general(
                query[j, :, view],
                key[:, view],
                (((1,), (1,)), ((), ())),
                preferred_element_type=jnp.float32,
            )
            decay = jnp.exp(
                jnp.minimum(key_level[number, :, 0:keys] - top[j, :, number : number + 1], 0.0)
            )
            coef = jnp.where(causal, decay * scores, 0.0) * (1.0 / math.sqrt(head_dim))
            denom_sum = jnp.sum(coef, axis=1, keepdims=True)
            numer_sum = jnp.dot(
                coef.astype(jnp.bfloat16), value[:, view], preferred_element_type=jnp.float32
            )
            for slot in range(2):
                keep[j, group, i, :, slot * head_dim : (slot + 1) * head_dim] = numer_sum[
                    slot * part : (slot + 1) * part, :
                ]
            denom[j, :, number : number + 1] = denom_sum[: 2 * part, :]
            reply[j, :, view] = numer_sum[2 * part :, :].astype(jnp.bfloat16)
            rest = denom_sum[2 * part :, :]
            for term in range(3):
                piece = rest.astype(jnp.bfloat16).astype(jnp.float32)
                rest = rest - piece
                extra = jnp.where(lane == 3 * i + term, piece, extra)
        reply[j, :, slice_width:] = extra.astype(jnp.bfloat16)

    def attend_slim(j):
        @pl.when(column == 0)
        def receive():
            arrive(query_slim.at[j, 2 * part :, :], slim_recv.at[j])

        attend(
            j,
            1,
            query_slim,
            key_slim,
            value_slim,
            chip * (2 * tokens) + key_lane[:, : 2 * tokens],
            chip_x,
            reply_slim,
        )

        @pl.when(column == 0)
        def answer():
            remote(
                reply_slim.at[j], from_near_slim.at[j], reply_send.at[0], reply_recv.at[0, j], 2
            )

    def attend_wide(j):
        arrive(query_wide.at[j, 2 * part :, :], wide_recv.at[j])
        attend(j, 0, query_wide, key_wide, value_wide, wide_place, query_chip, reply_wide)

        @pl.when(row == 0)
        def answer_far():
            remote(
                reply_wide.at[j], from_far_row.at[j], reply_send.at[1], reply_recv.at[1, j], 4
            )

        @pl.when(row == 1)
        def answer_near():
            remote(
                reply_wide.at[j], from_near_wide.at[j], reply_send.at[1], reply_recv.at[2, j], 2
            )

    def add_reply(j, group, number, source):
        arrive(source.at[j], reply_recv.at[number, j])
        extra = source[j, :, slice_width:].astype(jnp.float32)
        for i in range(2):
            for slot in range(2):
                view = slice(slot * head_dim, (slot + 1) * head_dim)
                keep[j, group, i, :, view] += source[
                    j, slot * part : (slot + 1) * part, i * head_dim : (i + 1) * head_dim
                ].astype(jnp.float32)
            number = 2 * group + i
            denom[j, :, number : number + 1] += (
                extra[:, 3 * i : 3 * i + 1]
                + extra[:, 3 * i + 1 : 3 * i + 2]
                + extra[:, 3 * i + 2 : 3 * i + 3]
            )

    def settle(j):
        @pl.when(row == 1)
        def add_row():
            add_reply(j, 1, 1, from_far_row)
            add_reply(j, 0, 2, from_near_wide)

        @pl.when(column == 1)
        def add_column():
            add_reply(j, 1, 0, from_near_slim)

        for group in range(2):
            for i in range(2):
                number = 2 * group + i
                for owner in (core, 1 - core):
                    divisor = denom[j, span_of(owner, part), :][:, number : number + 1]
                    value = (
                        keep[j, group, i, :, span_of(owner, head_dim)]
                        / jnp.maximum(jnp.abs(divisor), 1.0)
                    ).astype(jnp.bfloat16)
                    if owner is core:
                        first = bases[group] + core * slice_width + i * head_dim
                        mixer_in[j, :, pl.ds(pl.multiple_of(first, head_dim), head_dim)] = value
                    else:
                        first = group * slice_width + i * head_dim
                        mixed[j, :, first : first + head_dim] = value
            remote(
                mixed.at[j, :, pl.ds(group * slice_width, slice_width)],
                mixer_in.at[j, :, head_columns(bases[group], core)],
                mixed_send.at[0],
                mixed_recv.at[j],
                1,
            )

    def weigh():
        for slot in range(devices):
            told = info.at[peer(slot)] if slot else info.at[me]
            line = jnp.where(
                told[16:17, :].astype(jnp.int32) == me, told[18:19, :], 0.0
            ) + jnp.where(told[17:18, :].astype(jnp.int32) == me, told[19:20, :], 0.0)
            spread = jnp.where(along == across, jnp.broadcast_to(line, (tokens, tokens)), 0.0)
            weight_column = jnp.sum(spread, axis=1, keepdims=True)
            place = SLOT_ORDER.index(slot) * part
            for j in range(CHUNKS):
                slot_weight[j, place : place + part, :] = weight_column[
                    j * part : (j + 1) * part, :
                ]

    def slot_rows(slot):
        return pl.ds(SLOT_ORDER.index(slot) * part, part)

    def columns(half):
        return pl.ds(half * width, width)

    gathers = {}

    def gather(j, number, source, target, flip, half=None, begin=remote):
        view = slice(None) if half is None else columns(half)
        gathers[j, number] = begin(
            rows.at[j, slot_rows(source), view],
            rows.at[j, slot_rows(target), view],
            gather_send.at[0],
            gather_recv.at[j, number],
            flip,
        )

    def normalise(j):
        arrive(mixed.at[j], mixed_recv.at[j])
        if j == 0:
            large_loads[0].wait()
        span = slice(j * part, (j + 1) * part)
        mixer_out = mixer_in[j].astype(jnp.float32)
        square = jnp.mean(mixer_out * mixer_out, axis=1, keepdims=True)
        value = (
            updated[span, :].astype(jnp.float32)
            + mixer_out * lax.rsqrt(square + EPSILON) * mix_gain[...]
        ).astype(jnp.bfloat16)
        updated[span, :] = value
        value = value.astype(jnp.float32)
        square = jnp.mean(value * value, axis=1, keepdims=True)
        rows[j, 0:part, :] = (value * lax.rsqrt(square + EPSILON) * ffn_gain[...]).astype(
            jnp.bfloat16
        )

    def send_own(j, begin=remote):
        gather(j, 0, 0, 2, 2, 0, begin)
        gather(j, 1, 0, 4, 4, 1, begin)
        gather(j, 2, 0, 2, 2, 1, begin)
        gather(j, 3, 0, 4, 4, 0, begin)
        gather(j, 4, 0, 1, 1, None, begin)

    def attend_first():
        place = row_place[: 2 * part, :] + chip * (2 * tokens)
        causal = key_lane[:, : 2 * tokens] + chip * (2 * tokens) <= place
        for group, query, key, value in (
            (0, query_wide, key_wide, value_wide),
            (1, query_slim, key_slim, value_slim),
        ):
            for i in range(2):
                number = 2 * group + i
                view = slice(i * head_dim, (i + 1) * head_dim)
                scores = lax.dot_general(
                    query[0, : 2 * part, view],
                    key[: 2 * tokens, view],
                    (((1,), (1,)), ((), ())),
                    preferred_element_type=jnp.float32,
                )
                decay = jnp.exp(
                    jnp.minimum(
                        key_level[number, :, : 2 * tokens]
                        - top[0, : 2 * part, number : number + 1],
                        0.0,
                    )
                )
                coef = jnp.where(causal, decay * scores, 0.0) * (1.0 / math.sqrt(head_dim))
                denom[0, :, number : number + 1] = jnp.sum(coef, axis=1, keepdims=True)
                numer_sum = jnp.dot(
                    coef.astype(jnp.bfloat16),
                    value[: 2 * tokens, view],
                    preferred_element_type=jnp.float32,
                )
                for slot in range(2):
                    keep[0, group, i, :, slot * head_dim : (slot + 1) * head_dim] = numer_sum[
                        slot * part : (slot + 1) * part, :
                    ]

    def open_first():
        settle(0)
        normalise(0)
        for number in (0, 1, 2):
            gathers[0, number].start()

    def relay(j):
        gathers[j, 0].wait_recv()
        gather(j, 5, 2, 6, 4, 0)
        gathers[j, 1].wait_recv()
        gather(j, 6, 4, 6, 2, 1)
        gathers[j, 2].wait_recv()
        gather(j, 7, 2, 3, 1)
        gathers[j, 3].wait_recv()
        gather(j, 8, 4, 5, 1)

    def relay_last(j):
        gathers[j, 5].wait_recv()
        gathers[j, 6].wait_recv()
        gather(j, 9, 6, 7, 1)

    core_copies, hop_copies, last_copies = {}, {}, {}

    def compute(j):
        for number in (4, 7, 8, 9):
            gathers[j, number].wait_recv()
        if j == 0:
            large_loads[1].wait()
            large_loads[2].wait()
        for weight, total in ((gate, gate_sum), (up, up_sum)):
            total[...] = lax.dot_general(
                rows[j],
                weight[...],
                (((1,), (1,)), ((), ())),
                preferred_element_type=jnp.float32,
            )
        gate_val = gate_sum[...]
        hidden[...] = (gate_val / (1.0 + jnp.exp(-gate_val)) * up_sum[...]).astype(jnp.bfloat16)
        if j == 0:
            large_loads[3].wait()
        for half in range(HALVES):
            terms = (
                jnp.dot(hidden[...], down[:, columns(half)], preferred_element_type=jnp.float32)
                * slot_weight[j]
            ).astype(jnp.bfloat16)
            own[j % 2, half] = terms[:four, :]
            core_out[j, half] = terms[four:, :]
            core_copies[j, half] = remote(
                core_out.at[j, half],
                core_in.at[j, half],
                core_send.at[0],
                core_recv.at[j, half],
                1,
            )

    def first_hop(j, half):
        first, second = (2, 4) if half == 0 else (4, 2)
        core_copies[j, half].wait_recv()
        for slot in (6, first, second, 0):
            view = slot_rows(slot)
            both = own[j % 2, half, view, :].astype(jnp.float32) + core_in[
                j, half, view, :
            ].astype(jnp.float32)
            if slot in (0, second):
                keep[j, half, 0 if slot == 0 else 1] = both
                continue
            place = 1 if slot == 6 else 0
            hop_out[j, half, place] = both.astype(jnp.bfloat16)
            hop_copies[j, half, place] = remote(
                hop_out.at[j, half, place],
                hop_in.at[j, half, place],
                hop_send.at[0],
                hop_recv.at[j, half, place],
                first,
            )

    def second_hop(j, half):
        second = 4 if half == 0 else 2
        hop_copies[j, half, 1].wait_recv()
        last_out[j, half] = (
            keep[j, half, 1] + hop_in[j, half, 1].astype(jnp.float32)
        ).astype(jnp.bfloat16)
        last_copies[j, half] = remote(
            last_out.at[j, half],
            last_in.at[j, half],
            last_send.at[0],
            last_recv.at[j, half],
            second,
        )

    def finish(j, half):
        hop_copies[j, half, 0].wait_recv()
        last_copies[j, half].wait_recv()
        span = slice(j * part, (j + 1) * part)
        out[span, columns(half)] = (
            updated[span, columns(half)].astype(jnp.float32)
            + (
                keep[j, half, 0]
                + hop_in[j, half, 0].astype(jnp.float32)
                + last_in[j, half].astype(jnp.float32)
            )
        ).astype(jnp.bfloat16)

    def both_halves(step, j):
        for half in range(HALVES):
            step(j, half)

    arrive(key_wide, pair_recv.at[CHUNKS])
    for load in block_loads:
        load.wait()
    for j in range(CHUNKS):
        arrive(query_wide.at[j, : 2 * part, :], pair_recv.at[j])

    @pl.when(row == 1)
    def slim_early():
        for j in range(CHUNKS):
            attend_slim(j)

    send_own(0, prepared)

    @pl.when(chip == 0)
    def open_early():
        attend_first()
        open_first()

    weigh()
    arrive(key_wide, far_sem.at[1])
    attend_wide(0)
    attend_wide(1)

    @pl.when(row == 0)
    def slim_first():
        attend_slim(0)

    attend_wide(2)

    @pl.when(row == 0)
    def slim_second():
        attend_slim(1)

    attend_wide(3)

    @pl.when(row == 0)
    def slim_late():
        attend_slim(2)
        attend_slim(3)

    @pl.when(chip > 0)
    def open_late():
        open_first()

    gathers[0, 3].start()
    gathers[0, 4].start()
    settle(1)
    normalise(1)
    send_own(1)
    settle(2)
    settle(3)
    normalise(2)
    normalise(3)
    relay(0)
    send_own(2)
    relay(1)
    send_own(3)
    relay_last(0)
    compute(0)
    relay(2)
    relay_last(1)
    both_halves(first_hop, 0)
    compute(1)
    relay(3)
    relay_last(2)
    both_halves(first_hop, 1)
    compute(2)
    both_halves(second_hop, 0)
    relay_last(3)
    both_halves(first_hop, 2)
    compute(3)
    both_halves(second_hop, 1)
    both_halves(first_hop, 3)
    both_halves(second_hop, 2)
    both_halves(finish, 0)
    both_halves(finish, 1)
    both_halves(second_hop, 3)
    both_halves(finish, 2)
    both_halves(finish, 3)
    @pl.when(row == 0)
    def sent_keys():
        arrive(rows.at[0], far_sem.at[0])

    @pl.when(row == 1)
    def sent_wide_queries():
        arrive(key_wide, wide_send.at[0])

    @pl.when(column == 1)
    def sent_slim_queries():
        arrive(key_slim, slim_send.at[0])

    @pl.when(column == 0)
    def sent_slim_replies():
        arrive(reply_slim, reply_send.at[0])

    arrive(key_slim, pair_send.at[1])
    arrive(reply_wide, reply_send.at[1])
    for whole, flag in (
        (info.at[1:], info_sem),
        (key_wide, pair_send),
        (mixed, mixed_send),
        (rows.at[:, part:, :], gather_send),
        (core_out, core_send),
        (hop_out, hop_send),
        (last_out, last_send),
    ):
        arrive(whole, flag.at[0])


def fused_block(*operands):
    queries, gates, gate_weight = operands[0], operands[4], operands[10]
    tokens, model_width = queries.shape
    devices = gates.shape[0]
    head_dim = model_width // devices
    hidden_width = gate_weight.shape[0]
    part = tokens // CHUNKS
    width = model_width // HALVES
    batch = devices * part
    near = pl.BlockSpec(memory_space=pltpu.VMEM)
    far = pl.BlockSpec(memory_space=pl.ANY)

    def space(*shape, kind=jnp.bfloat16):
        return pltpu.VMEM(shape, kind)

    def flags(*shape):
        return [pltpu.SemaphoreType.DMA((1,)), pltpu.SemaphoreType.DMA(shape)]

    return pl.pallas_call(
        fused_kernel,
        out_shape=pltpu.VMEM((tokens, model_width), jnp.bfloat16),
        in_specs=[far] * 13,
        out_specs=near,
        scratch_shapes=[
            space(devices, tokens, kind=jnp.float32),
            space(devices, tokens, kind=jnp.float32),
            space(2, tokens, kind=jnp.int32),
            space(2, tokens, kind=jnp.float32),
            space(1, model_width, kind=jnp.float32),
            space(1, model_width, kind=jnp.float32),
            space(devices, 24, tokens, kind=jnp.float32),
            space(devices, devices, tokens, kind=jnp.float32),
            space(devices, devices, tokens, kind=jnp.float32),
            space(4, 1, 4 * tokens, kind=jnp.float32),
            space(CHUNKS, 4 * part, 4, kind=jnp.float32),
            space(CHUNKS, batch, 1, kind=jnp.float32),
            space(CHUNKS, 4 * part, 2 * head_dim),
            space(CHUNKS, 4 * part, 2 * head_dim),
            space(4 * tokens, 2 * head_dim),
            space(4 * tokens, 2 * head_dim),
            space(2 * tokens, 2 * head_dim),
            space(2 * tokens, 2 * head_dim),
        ]
        + [space(CHUNKS, 2 * part, 2 * head_dim + tokens)] * 5
        + [
            space(CHUNKS, 2 * part, 4, kind=jnp.float32),
            space(CHUNKS, part, 4 * head_dim),
            space(CHUNKS, part, model_width),
            space(tokens, model_width),
            space(CHUNKS, batch, model_width),
            space(*gate_weight.shape),
            space(*gate_weight.shape),
            space(*gate_weight.shape),
            space(batch, hidden_width, kind=jnp.float32),
            space(batch, hidden_width, kind=jnp.float32),
            space(batch, hidden_width),
            space(2, HALVES, batch // 2, width),
            space(CHUNKS, HALVES, batch // 2, width),
            space(CHUNKS, HALVES, batch // 2, width),
            space(CHUNKS, HALVES, 2, part, width),
            space(CHUNKS, HALVES, 2, part, width),
            space(CHUNKS, HALVES, 2, part, width, kind=jnp.float32),
            space(CHUNKS, HALVES, part, width),
            space(CHUNKS, HALVES, part, width),
            pltpu.SemaphoreType.DMA((14 + 2 * CHUNKS,)),
            pltpu.SemaphoreType.DMA((2,)),
            pltpu.SemaphoreType.DMA((2,)),
            pltpu.SemaphoreType.DMA((CHUNKS + 1,)),
            pltpu.SemaphoreType.DMA((2,)),
        ]
        + flags(CHUNKS)
        + flags(CHUNKS)
        + [pltpu.SemaphoreType.DMA((2,)), pltpu.SemaphoreType.DMA((3, CHUNKS))]
        + flags(CHUNKS)
        + flags(CHUNKS, 10)
        + flags(CHUNKS, HALVES)
        + flags(CHUNKS, HALVES, 2)
        + flags(CHUNKS, HALVES),
        compiler_params=pltpu.CompilerParams(
            collective_id=1, has_side_effects=True, vmem_limit_bytes=VMEM_BYTES
        ),
    )(*operands)


def shards(
    queries,
    key_vectors,
    value_vectors,
    residual_in,
    input_logit,
    forget_logit,
    mix_gain,
    ffn_gain,
    expert_gate,
    expert_up,
    expert_down,
    routes,
    route_weight,
):
    tokens, model_width = queries.shape
    head_count = input_logit.shape[0]
    head_dim = model_width // head_count
    devices = lax.axis_size("seq")
    group = devices // head_count
    group_width = model_width // devices
    if devices == 8 and head_count == 8:
        return fused_block(
            queries,
            key_vectors,
            value_vectors,
            residual_in,
            input_logit,
            forget_logit,
            jnp.transpose(routes),
            jnp.transpose(route_weight),
            mix_gain.reshape(1, -1),
            ffn_gain.reshape(1, -1),
            jnp.transpose(expert_gate[0]),
            jnp.transpose(expert_up[0]),
            expert_down[0],
        )

    capacity = 4 * tokens // devices
    flat_routes = routes.reshape(-1)
    matches = (flat_routes[:, None] == jnp.arange(devices, dtype=jnp.int32)[None, :]).astype(
        jnp.int32
    )
    before = jnp.cumsum(matches, axis=0) - matches
    position = jnp.sum(before * matches, axis=1)
    position = position.reshape(tokens, 2)
    slot_index = (flat_routes * capacity + position.reshape(-1)).reshape(tokens, 2)
    notes = jnp.stack(
        (jnp.repeat(input_logit, group, axis=0), jnp.repeat(forget_logit, group, axis=0)), axis=1
    )
    def columns_of(width, share):
        return lambda ref, other: ref.at[
            :, pl.ds(pl.multiple_of((other // share) * width, width), width)
        ]

    def rows_from(ref, origin):
        return ref.at[pl.ds(pl.multiple_of(origin * tokens, tokens), tokens), :]

    def entry(ref, other):
        return ref.at[other]

    head_columns = columns_of(head_dim, group)
    own_columns = columns_of(group_width, 1)
    tall = devices * tokens
    told, key_all, query_all, value_all = exchange(
        (
            (entry, entry),
            (head_columns, rows_from),
            (head_columns, rows_from),
            (own_columns, rows_from),
        ),
        devices,
        2,
        (notes, key_vectors, queries, value_vectors),
        (
            jax.ShapeDtypeStruct(notes.shape, jnp.float32),
            jax.ShapeDtypeStruct((tall, head_dim), jnp.bfloat16),
            jax.ShapeDtypeStruct((tall, head_dim), jnp.bfloat16),
            jax.ShapeDtypeStruct((tall, group_width), jnp.bfloat16),
        ),
    )
    mixed = head_mix(
        query_all, key_all, value_all, told[:, 0].reshape(-1), told[:, 1].reshape(-1)
    ).astype(jnp.bfloat16)
    (mixer_out,) = exchange(
        ((rows_from, own_columns),),
        devices,
        3,
        (mixed,),
        (jax.ShapeDtypeStruct((tokens, model_width), jnp.bfloat16),),
    )
    mixer_out = mixer_out.astype(jnp.float32)
    mixer_square = jnp.mean(mixer_out * mixer_out, axis=1, keepdims=True)
    updated = (
        residual_in.astype(jnp.float32) + mixer_out * lax.rsqrt(mixer_square + EPSILON) * mix_gain
    ).astype(jnp.bfloat16)
    updated_float = updated.astype(jnp.float32)
    updated_square = jnp.mean(updated_float * updated_float, axis=1, keepdims=True)
    normed = (updated_float * lax.rsqrt(updated_square + EPSILON) * ffn_gain).astype(jnp.bfloat16)
    columns = jnp.arange(devices * capacity, dtype=jnp.int32)
    pick_first = (slot_index[:, 0:1] == columns[None, :]).astype(jnp.bfloat16)
    pick_second = (slot_index[:, 1:2] == columns[None, :]).astype(jnp.bfloat16)
    spread = jnp.einsum(
        "tc,td->cd", pick_first + pick_second, normed, preferred_element_type=jnp.float32
    ).astype(jnp.bfloat16)
    outbound = spread.reshape(devices, capacity, model_width)
    block_in = lax.all_to_all(outbound, "seq", split_axis=0, concat_axis=0, tiled=True)
    row_block = block_in.reshape(-1, model_width)
    gate_val = jnp.dot(row_block, expert_gate[0], preferred_element_type=jnp.float32)
    up_val = jnp.dot(row_block, expert_up[0], preferred_element_type=jnp.float32)
    hidden = (jax.nn.silu(gate_val) * up_val).astype(jnp.bfloat16)
    result = jnp.dot(hidden, expert_down[0], preferred_element_type=jnp.float32).astype(
        jnp.bfloat16
    )
    inbound = lax.all_to_all(
        result.reshape(block_in.shape), "seq", split_axis=0, concat_axis=0, tiled=True
    )
    flat_back = inbound.reshape(devices * capacity, model_width)
    first_out = jnp.dot(pick_first, flat_back, preferred_element_type=jnp.float32)
    second_out = jnp.dot(pick_second, flat_back, preferred_element_type=jnp.float32)
    expert_mix = route_weight[:, 0:1] * first_out + route_weight[:, 1:2] * second_out
    return (updated_float + expert_mix).astype(jnp.bfloat16)


def solution(mesh):
    return jax.shard_map(
        shards,
        mesh=mesh,
        in_specs=(
            P(("batch", "seq"), None),
            P(("batch", "seq"), None),
            P(("batch", "seq"), None),
            P(("batch", "seq"), None),
            P(None, ("batch", "seq")),
            P(None, ("batch", "seq")),
            P(),
            P(),
            P("seq", None, None),
            P("seq", None, None),
            P("seq", None, None),
            P(("batch", "seq"), None),
            P(("batch", "seq"), None),
        ),
        out_specs=P(("batch", "seq"), None),
        check_vma=False,
    )
```

```python
import functools
import math

import jax
import jax.numpy as jnp
from jax import lax
from jax.experimental import pallas as pl
from jax.experimental.pallas import tpu as pltpu
from jax.sharding import PartitionSpec as P

EPSILON = 1e-06
CHUNKS = 4
HALVES = 2
FLIPS = (6, 4, 2, 7, 5, 3, 1)
SLOT_ORDER = (0, 2, 4, 6, 1, 3, 5, 7)
VMEM_BYTES = 64 * 1024 * 1024 - 1280 * 1024
LOW = -1e30


def exchange_kernel(moves, devices, *refs):
    count = len(moves)
    sources, targets = refs[:count], refs[count : 2 * count]
    send_sem, recv_sem, local_sem = refs[2 * count :]
    me = lax.axis_index("seq")
    others = [lax.rem(me + step, devices) for step in range(1, devices)]
    barrier = pltpu.get_barrier_semaphore()
    for other in others:
        pl.semaphore_signal(
            barrier, inc=1, device_id={"seq": other}, device_id_type=pl.DeviceIdType.MESH
        )
    pl.semaphore_wait(barrier, devices - 1)
    copies = []
    for i, (take, put) in enumerate(moves):
        for step, other in enumerate(others):
            copies.append(
                pltpu.make_async_remote_copy(
                    src_ref=take(sources[i], other),
                    dst_ref=put(targets[i], me),
                    send_sem=send_sem.at[i, step],
                    recv_sem=recv_sem.at[i, step],
                    device_id={"seq": other},
                    device_id_type=pl.DeviceIdType.MESH,
                )
            )
            copies[-1].start()
    for i, (take, put) in enumerate(moves):
        copies.append(
            pltpu.make_async_copy(take(sources[i], me), put(targets[i], me), local_sem.at[i])
        )
        copies[-1].start()
    for copy in copies:
        copy.wait()


def exchange(moves, devices, number, sources, shapes):
    far = pl.BlockSpec(memory_space=pl.ANY)
    count = len(moves)
    return pl.pallas_call(
        functools.partial(exchange_kernel, moves, devices),
        out_shape=shapes,
        in_specs=[far] * count,
        out_specs=[far] * count,
        scratch_shapes=[
            pltpu.SemaphoreType.DMA((count, devices - 1)),
            pltpu.SemaphoreType.DMA((count, devices - 1)),
            pltpu.SemaphoreType.DMA((count,)),
        ],
        compiler_params=pltpu.CompilerParams(collective_id=number, has_side_effects=True),
    )(*sources)


def head_mix(query, key, value, input_gate, forget_gate):
    positions, head_dim = query.shape
    cumul_log = jnp.cumsum(jax.nn.log_sigmoid(forget_gate))
    level = input_gate - cumul_log
    top = lax.cummax(level, axis=0)
    scores = lax.dot_general(
        query, key, (((1,), (1,)), ((), ())), preferred_element_type=jnp.float32
    )
    causal = jnp.arange(positions)[:, None] >= jnp.arange(positions)[None, :]
    decay = jnp.exp(jnp.minimum(level[None, :] - top[:, None], 0.0))
    coef = jnp.where(causal, decay * scores, 0.0) * (1.0 / math.sqrt(head_dim))
    denom_sum = jnp.sum(coef, axis=1, keepdims=True)
    numer_sum = jnp.dot(coef.astype(jnp.bfloat16), value, preferred_element_type=jnp.float32)
    return numer_sum / jnp.maximum(jnp.abs(denom_sum), 1.0)


def fused_kernel(
    query_far,
    key_far,
    value_far,
    residual_far,
    input_far,
    forget_far,
    routes_far,
    weights_far,
    mix_far,
    ffn_far,
    gate_far,
    up_far,
    down_far,
    out,
    input_gate,
    forget_gate,
    routes,
    weights,
    mix_gain,
    ffn_gain,
    info,
    level,
    peak_before,
    key_level,
    top,
    slot_weight,
    query_wide,
    query_slim,
    key_wide,
    value_wide,
    key_slim,
    value_slim,
    reply_wide,
    reply_slim,
    from_far_row,
    from_near_wide,
    from_near_slim,
    denom,
    denom_out,
    denom_in,
    mixed,
    mixer_in,
    updated,
    rows,
    gate,
    up,
    down,
    gate_sum,
    up_sum,
    hidden,
    own,
    core_out,
    core_in,
    hop_out,
    hop_in,
    keep,
    last_out,
    last_in,
    load_sem,
    info_sem,
    pair_send,
    pair_recv,
    far_sem,
    wide_send,
    wide_recv,
    slim_send,
    slim_recv,
    reply_send,
    reply_recv,
    denom_send,
    denom_recv,
    mixed_send,
    mixed_recv,
    gather_send,
    gather_recv,
    core_send,
    core_recv,
    hop_send,
    hop_recv,
    last_send,
    last_recv,
):
    me = lax.axis_index("seq")
    heads, tokens = input_gate.shape
    devices = heads
    model_width = out.shape[1]
    head_dim = model_width // heads
    part = tokens // CHUNKS
    width = model_width // HALVES
    four = devices // 2 * part
    slice_width = 2 * head_dim
    core = lax.rem(me, 2)
    column = lax.rem(lax.div(me, 2), 2)
    row = lax.div(me, 4)
    chip = lax.div(me, 2)
    chip_x = chip + 1 - 2 * column
    chip_y = chip + 2 - 4 * row
    key_chip = chip_x * (1 - row) + chip_y * row
    query_chip = chip_y * (1 - row) + chip_x * row
    wide_base = (1 - row) * width
    slim_base = row * width
    bases = (wide_base, slim_base)

    def peer(flip):
        total = 0
        for bit in (1, 2, 4):
            own_bit = lax.rem(lax.div(me, bit), 2)
            total = total + bit * ((1 - own_bit) if flip & bit else own_bit)
        return total

    def arrive(whole, flag):
        pltpu.make_async_copy(whole, whole, flag).wait()

    def prepared(source, target, send_sem, recv_sem, flip):
        return pltpu.make_async_remote_copy(
            src_ref=source,
            dst_ref=target,
            send_sem=send_sem,
            recv_sem=recv_sem,
            device_id={"seq": peer(flip)},
            device_id_type=pl.DeviceIdType.MESH,
        )

    def remote(*arguments):
        copy = prepared(*arguments)
        copy.start()
        return copy

    def span_of(index, count, first=0):
        return pl.ds(pl.multiple_of(index * count + first, count), count)

    def head_columns(base, owner):
        return pl.ds(pl.multiple_of(base + owner * slice_width, slice_width), slice_width)

    def core_of(flip):
        return 1 - core if flip % 2 else core

    barrier = pltpu.get_barrier_semaphore()
    for flip in FLIPS:
        pl.semaphore_signal(
            barrier,
            inc=1,
            device_id={"seq": peer(flip)},
            device_id_type=pl.DeviceIdType.MESH,
        )
    small = (
        (input_far, input_gate),
        (forget_far, forget_gate),
        (routes_far, routes),
        (weights_far, weights),
        (mix_far, mix_gain),
        (ffn_far, ffn_gain),
    )
    blocks = tuple(
        (far.at[:, head_columns(base, core)], target.at[span_of(core, tokens), :])
        for base, far, target in (
            (wide_base, key_far, key_wide),
            (wide_base, value_far, value_wide),
            (slim_base, key_far, key_slim),
            (slim_base, value_far, value_slim),
        )
    ) + tuple(
        (
            query_far.at[pl.ds(j * part, part), head_columns(base, core)],
            target.at[j, span_of(core, part), :],
        )
        for j in range(CHUNKS)
        for base, target in ((wide_base, query_wide), (slim_base, query_slim))
    )
    large = ((residual_far, updated), (gate_far, gate), (up_far, up), (down_far, down))
    loads = [
        pltpu.make_async_copy(source, target, load_sem.at[i])
        for i, (source, target) in enumerate(small + blocks + large)
    ]
    small_loads, block_loads, large_loads = loads[:6], loads[6:18], loads[18:]
    for load in small_loads + block_loads:
        load.start()
    for load in small_loads:
        load.wait()
    forget = forget_gate[...]
    info[me, 0:8, :] = input_gate[...]
    info[me, 8:16, :] = -(jnp.maximum(-forget, 0.0) + jnp.log1p(jnp.exp(-jnp.abs(forget))))
    info[me, 16:18, :] = routes[...].astype(jnp.float32)
    info[me, 18:20, :] = weights[...]
    pl.semaphore_wait(barrier, devices - 1)

    for flip in (6, 4, 2, 1):
        remote(info.at[me], info.at[me], info_sem.at[0], info_sem.at[1], flip)

    @pl.when(row == 0)
    def send_keys():
        for far, target in ((key_far, key_wide), (value_far, value_wide)):
            for flip, base in ((2, wide_base), (4, slim_base), (3, wide_base), (5, slim_base)):
                remote(
                    far.at[:, head_columns(base, core_of(flip))],
                    target.at[span_of(core, tokens, 2 * tokens), :],
                    far_sem.at[0],
                    far_sem.at[1],
                    flip,
                )

    @pl.when(column == 1)
    def send_slim_queries():
        for j in range(CHUNKS):
            for flip in (2, 3):
                remote(
                    query_far.at[pl.ds(j * part, part), head_columns(slim_base, core_of(flip))],
                    query_slim.at[j, span_of(core, part, 2 * part), :],
                    slim_send.at[0],
                    slim_recv.at[j],
                    flip,
                )

    @pl.when(row == 1)
    def send_wide_queries():
        for j in range(CHUNKS):
            for flip, base in ((2, wide_base), (4, slim_base), (3, wide_base), (5, slim_base)):
                remote(
                    query_far.at[pl.ds(j * part, part), head_columns(base, core_of(flip))],
                    query_wide.at[j, span_of(core, part, 2 * part), :],
                    wide_send.at[0],
                    wide_recv.at[j],
                    flip,
                )

    for base, far, target in (
        (wide_base, key_far, key_wide),
        (wide_base, value_far, value_wide),
        (slim_base, key_far, key_slim),
        (slim_base, value_far, value_slim),
    ):
        remote(
            far.at[:, head_columns(base, 1 - core)],
            target.at[span_of(core, tokens), :],
            pair_send.at[0],
            pair_recv.at[CHUNKS],
            1,
        )
    for j in range(CHUNKS):
        for base, target in ((wide_base, query_wide), (slim_base, query_slim)):
            remote(
                query_far.at[pl.ds(j * part, part), head_columns(base, 1 - core)],
                target.at[j, span_of(core, part), :],
                pair_send.at[1],
                pair_recv.at[j],
                1,
            )
    for load in large_loads:
        load.start()

    arrive(info.at[:4], info_sem.at[1])
    for flip in (2, 4, 6):
        told = info.at[peer(flip)]
        remote(told, told, info_sem.at[2], info_sem.at[3], 1)
    arrive(info.at[:3], info_sem.at[3])
    across = lax.broadcasted_iota(jnp.int32, (tokens, tokens), 0)
    along = lax.broadcasted_iota(jnp.int32, (tokens, tokens), 1)
    local_sum = jnp.dot(
        info[:, 8:16, :].reshape(devices * heads, tokens),
        (across <= along).astype(jnp.float32),
        precision=lax.Precision.HIGHEST,
        preferred_element_type=jnp.float32,
    )
    before = jnp.zeros((heads, 1), jnp.float32)
    peak = jnp.full((heads, 1), LOW, jnp.float32)
    for block in range(devices):
        lines = local_sum[block * heads : (block + 1) * heads, :]
        level_lines = info[block, 0:8, :] - (lines + before)
        before = before + lines[:, tokens - 1 : tokens]
        level[block] = level_lines
        peak_before[block] = jnp.broadcast_to(peak, (heads, tokens))
        peak = jnp.maximum(peak, jnp.max(level_lines, axis=1, keepdims=True))
    for group, first_chip in ((0, query_chip), (1, chip_x)):
        for i in range(2):
            head = (row if group else 1 - row) * (heads // 2) + 2 * core + i
            for slot in range(4):
                block = 2 * (chip if slot < 2 else first_chip) + slot % 2
                line = level[block, pl.ds(head, 1), :]
                if slot < 2:
                    key_level[2 * group + i, :, slot * tokens : (slot + 1) * tokens] = line
                spread = jnp.where(along <= across, jnp.broadcast_to(line, (tokens, tokens)), LOW)
                tops = jnp.maximum(
                    jnp.max(spread, axis=1, keepdims=True),
                    peak_before[block, pl.ds(head, 1), :][:, 0:1],
                )
                for j in range(CHUNKS):
                    top[j, slot * part : (slot + 1) * part, 2 * group + i : 2 * group + i + 1] = (
                        tops[j * part : (j + 1) * part, :]
                    )
            if group == 0:
                for slot in (2, 3):
                    key_level[i, :, slot * tokens : (slot + 1) * tokens] = level[
                        2 * key_chip + slot % 2, pl.ds(head, 1), :
                    ]

    query_row = lax.broadcasted_iota(jnp.int32, (4 * part, 1), 0)
    row_block = lax.shift_right_logical(query_row, part.bit_length() - 1)
    foreign_row = row_block >= 2
    row_place = (
        jnp.where(foreign_row, row_block - 2, row_block) * (tokens - part)
        + query_row
        - jnp.where(foreign_row, 2 * part, 0)
    )
    diagonal = across[: 2 * part, :] == along[: 2 * part, :]
    key_lane = lax.broadcasted_iota(jnp.int32, (1, 4 * tokens), 1)
    wide_place = jnp.where(
        key_lane < 2 * tokens,
        chip * (2 * tokens) + key_lane,
        key_chip * (2 * tokens) + key_lane - 2 * tokens,
    )

    def attend(j, group, query, key, value, key_place, foreign_chip, reply):
        place = row_place + j * part + jnp.where(foreign_row, foreign_chip, chip) * (2 * tokens)
        causal = key_place <= place
        keys = key.shape[0]
        for i in range(2):
            number = 2 * group + i
            view = slice(i * head_dim, (i + 1) * head_dim)
            scores = lax.dot_general(
                query[j, :, view],
                key[:, view],
                (((1,), (1,)), ((), ())),
                preferred_element_type=jnp.float32,
            )
            decay = jnp.exp(
                jnp.minimum(key_level[number, :, 0:keys] - top[j, :, number : number + 1], 0.0)
            )
            coef = jnp.where(causal, decay * scores, 0.0) * (1.0 / math.sqrt(head_dim))
            denom_sum = jnp.sum(coef, axis=1, keepdims=True)
            numer_sum = jnp.dot(
                coef.astype(jnp.bfloat16), value[:, view], preferred_element_type=jnp.float32
            )
            for slot in range(2):
                keep[j, group, i, :, slot * head_dim : (slot + 1) * head_dim] = numer_sum[
                    slot * part : (slot + 1) * part, :
                ]
            denom[j, :, number : number + 1] = denom_sum[: 2 * part, :]
            reply[j, :, view] = numer_sum[2 * part :, :].astype(jnp.bfloat16)
            denom_out[group, j, i : i + 1, :] = jnp.sum(
                jnp.where(diagonal, denom_sum[2 * part :, :], 0.0), axis=0, keepdims=True
            )

    def answer(j, group, number, reply, target, flip):
        remote(
            reply.at[j], target.at[j], reply_send.at[group], reply_recv.at[number, j], flip
        )
        remote(
            denom_out.at[group, j],
            denom_in.at[number, j],
            denom_send.at[group],
            denom_recv.at[number, j],
            flip,
        )

    def attend_slim(j):
        @pl.when(column == 0)
        def receive():
            arrive(query_slim.at[j, 2 * part :, :], slim_recv.at[j])

        attend(
            j,
            1,
            query_slim,
            key_slim,
            value_slim,
            chip * (2 * tokens) + key_lane[:, : 2 * tokens],
            chip_x,
            reply_slim,
        )

        @pl.when(column == 0)
        def answer_slim():
            answer(j, 1, 0, reply_slim, from_near_slim, 2)

    def attend_wide(j):
        arrive(query_wide.at[j, 2 * part :, :], wide_recv.at[j])
        attend(j, 0, query_wide, key_wide, value_wide, wide_place, query_chip, reply_wide)

        @pl.when(row == 0)
        def answer_far():
            answer(j, 0, 1, reply_wide, from_far_row, 4)

        @pl.when(row == 1)
        def answer_near():
            answer(j, 0, 2, reply_wide, from_near_wide, 2)

    def add_reply(j, group, number, source):
        arrive(source.at[j], reply_recv.at[number, j])
        arrive(denom_in.at[number, j], denom_recv.at[number, j])
        for i in range(2):
            for slot in range(2):
                view = slice(slot * head_dim, (slot + 1) * head_dim)
                keep[j, group, i, :, view] += source[
                    j, slot * part : (slot + 1) * part, i * head_dim : (i + 1) * head_dim
                ].astype(jnp.float32)
            place = 2 * group + i
            denom[j, :, place : place + 1] += jnp.sum(
                jnp.where(diagonal, denom_in[number, j, i : i + 1, :], 0.0),
                axis=1,
                keepdims=True,
            )

    def settle(j):
        @pl.when(row == 1)
        def add_row():
            add_reply(j, 1, 1, from_far_row)
            add_reply(j, 0, 2, from_near_wide)

        @pl.when(column == 1)
        def add_column():
            add_reply(j, 1, 0, from_near_slim)

        for group in range(2):
            for i in range(2):
                number = 2 * group + i
                for owner in (core, 1 - core):
                    divisor = denom[j, span_of(owner, part), :][:, number : number + 1]
                    value = (
                        keep[j, group, i, :, span_of(owner, head_dim)]
                        / jnp.maximum(jnp.abs(divisor), 1.0)
                    ).astype(jnp.bfloat16)
                    if owner is core:
                        first = bases[group] + core * slice_width + i * head_dim
                        mixer_in[j, :, pl.ds(pl.multiple_of(first, head_dim), head_dim)] = value
                    else:
                        first = group * slice_width + i * head_dim
                        mixed[j, :, first : first + head_dim] = value
            remote(
                mixed.at[j, :, pl.ds(group * slice_width, slice_width)],
                mixer_in.at[j, :, head_columns(bases[group], core)],
                mixed_send.at[0],
                mixed_recv.at[j],
                1,
            )

    def weigh():
        for slot in range(devices):
            told = info.at[peer(slot)] if slot else info.at[me]
            line = jnp.where(
                told[16:17, :].astype(jnp.int32) == me, told[18:19, :], 0.0
            ) + jnp.where(told[17:18, :].astype(jnp.int32) == me, told[19:20, :], 0.0)
            spread = jnp.where(along == across, jnp.broadcast_to(line, (tokens, tokens)), 0.0)
            weight_column = jnp.sum(spread, axis=1, keepdims=True)
            place = SLOT_ORDER.index(slot) * part
            for j in range(CHUNKS):
                slot_weight[j, place : place + part, :] = weight_column[
                    j * part : (j + 1) * part, :
                ]

    def slot_rows(slot):
        return pl.ds(SLOT_ORDER.index(slot) * part, part)

    def columns(half):
        return pl.ds(half * width, width)

    gathers = {}

    def gather(j, number, source, target, flip, half=None, begin=remote):
        view = slice(None) if half is None else columns(half)
        gathers[j, number] = begin(
            rows.at[j, slot_rows(source), view],
            rows.at[j, slot_rows(target), view],
            gather_send.at[0],
            gather_recv.at[j, number],
            flip,
        )

    def normalise(j):
        arrive(mixed.at[j], mixed_recv.at[j])
        if j == 0:
            large_loads[0].wait()
        span = slice(j * part, (j + 1) * part)
        mixer_out = mixer_in[j].astype(jnp.float32)
        square = jnp.mean(mixer_out * mixer_out, axis=1, keepdims=True)
        value = (
            updated[span, :].astype(jnp.float32)
            + mixer_out * lax.rsqrt(square + EPSILON) * mix_gain[...]
        ).astype(jnp.bfloat16)
        updated[span, :] = value
        value = value.astype(jnp.float32)
        square = jnp.mean(value * value, axis=1, keepdims=True)
        rows[j, 0:part, :] = (value * lax.rsqrt(square + EPSILON) * ffn_gain[...]).astype(
            jnp.bfloat16
        )

    def send_own(j, begin=remote):
        gather(j, 0, 0, 2, 2, 0, begin)
        gather(j, 1, 0, 4, 4, 1, begin)
        gather(j, 2, 0, 2, 2, 1, begin)
        gather(j, 3, 0, 4, 4, 0, begin)
        gather(j, 4, 0, 1, 1, None, begin)

    def attend_first():
        place = row_place[: 2 * part, :] + chip * (2 * tokens)
        causal = key_lane[:, : 2 * tokens] + chip * (2 * tokens) <= place
        for group, query, key, value in (
            (0, query_wide, key_wide, value_wide),
            (1, query_slim, key_slim, value_slim),
        ):
            for i in range(2):
                number = 2 * group + i
                view = slice(i * head_dim, (i + 1) * head_dim)
                scores = lax.dot_general(
                    query[0, : 2 * part, view],
                    key[: 2 * tokens, view],
                    (((1,), (1,)), ((), ())),
                    preferred_element_type=jnp.float32,
                )
                decay = jnp.exp(
                    jnp.minimum(
                        key_level[number, :, : 2 * tokens]
                        - top[0, : 2 * part, number : number + 1],
                        0.0,
                    )
                )
                coef = jnp.where(causal, decay * scores, 0.0) * (1.0 / math.sqrt(head_dim))
                denom[0, :, number : number + 1] = jnp.sum(coef, axis=1, keepdims=True)
                numer_sum = jnp.dot(
                    coef.astype(jnp.bfloat16),
                    value[: 2 * tokens, view],
                    preferred_element_type=jnp.float32,
                )
                for slot in range(2):
                    keep[0, group, i, :, slot * head_dim : (slot + 1) * head_dim] = numer_sum[
                        slot * part : (slot + 1) * part, :
                    ]

    def open_first():
        settle(0)
        normalise(0)
        for number in (0, 1, 2):
            gathers[0, number].start()

    def relay(j):
        gathers[j, 0].wait_recv()
        gather(j, 5, 2, 6, 4, 0)
        gathers[j, 1].wait_recv()
        gather(j, 6, 4, 6, 2, 1)
        gathers[j, 2].wait_recv()
        gather(j, 7, 2, 3, 1)
        gathers[j, 3].wait_recv()
        gather(j, 8, 4, 5, 1)

    def relay_last(j):
        gathers[j, 5].wait_recv()
        gathers[j, 6].wait_recv()
        gather(j, 9, 6, 7, 1)

    core_copies, hop_copies, last_copies = {}, {}, {}

    def compute(j):
        for number in (4, 7, 8, 9):
            gathers[j, number].wait_recv()
        if j == 0:
            large_loads[1].wait()
            large_loads[2].wait()
        for weight, total in ((gate, gate_sum), (up, up_sum)):
            total[...] = lax.dot_general(
                rows[j],
                weight[...],
                (((1,), (1,)), ((), ())),
                preferred_element_type=jnp.float32,
            )
        gate_val = gate_sum[...]
        hidden[...] = (gate_val / (1.0 + jnp.exp(-gate_val)) * up_sum[...]).astype(jnp.bfloat16)
        if j == 0:
            large_loads[3].wait()
        for half in range(HALVES):
            terms = (
                jnp.dot(hidden[...], down[:, columns(half)], preferred_element_type=jnp.float32)
                * slot_weight[j]
            ).astype(jnp.bfloat16)
            own[j % 2, half] = terms[:four, :]
            core_out[j, half] = terms[four:, :]
            core_copies[j, half] = remote(
                core_out.at[j, half],
                core_in.at[j, half],
                core_send.at[0],
                core_recv.at[j, half],
                1,
            )

    def first_hop(j, half):
        first, second = (2, 4) if half == 0 else (4, 2)
        core_copies[j, half].wait_recv()
        for slot in (6, first, second, 0):
            view = slot_rows(slot)
            both = own[j % 2, half, view, :].astype(jnp.float32) + core_in[
                j, half, view, :
            ].astype(jnp.float32)
            if slot in (0, second):
                keep[j, half, 0 if slot == 0 else 1] = both
                continue
            place = 1 if slot == 6 else 0
            hop_out[j, half, place] = both.astype(jnp.bfloat16)
            hop_copies[j, half, place] = remote(
                hop_out.at[j, half, place],
                hop_in.at[j, half, place],
                hop_send.at[0],
                hop_recv.at[j, half, place],
                first,
            )

    def second_hop(j, half):
        second = 4 if half == 0 else 2
        hop_copies[j, half, 1].wait_recv()
        last_out[j, half] = (
            keep[j, half, 1] + hop_in[j, half, 1].astype(jnp.float32)
        ).astype(jnp.bfloat16)
        last_copies[j, half] = remote(
            last_out.at[j, half],
            last_in.at[j, half],
            last_send.at[0],
            last_recv.at[j, half],
            second,
        )

    def finish(j, half):
        hop_copies[j, half, 0].wait_recv()
        last_copies[j, half].wait_recv()
        span = slice(j * part, (j + 1) * part)
        out[span, columns(half)] = (
            updated[span, columns(half)].astype(jnp.float32)
            + (
                keep[j, half, 0]
                + hop_in[j, half, 0].astype(jnp.float32)
                + last_in[j, half].astype(jnp.float32)
            )
        ).astype(jnp.bfloat16)

    def both_halves(step, j):
        for half in range(HALVES):
            step(j, half)

    arrive(key_wide, pair_recv.at[CHUNKS])
    for load in block_loads:
        load.wait()
    for j in range(CHUNKS):
        arrive(query_wide.at[j, : 2 * part, :], pair_recv.at[j])

    @pl.when(row == 1)
    def slim_early():
        for j in range(CHUNKS):
            attend_slim(j)

    send_own(0, prepared)

    @pl.when(chip == 0)
    def open_early():
        attend_first()
        open_first()

    weigh()
    arrive(key_wide, far_sem.at[1])
    attend_wide(0)
    attend_wide(1)

    @pl.when(row == 0)
    def slim_first():
        attend_slim(0)

    attend_wide(2)

    @pl.when(row == 0)
    def slim_second():
        attend_slim(1)

    attend_wide(3)

    @pl.when(row == 0)
    def slim_late():
        attend_slim(2)
        attend_slim(3)

    @pl.when(chip > 0)
    def open_late():
        open_first()

    gathers[0, 3].start()
    gathers[0, 4].start()
    settle(1)
    normalise(1)
    send_own(1)
    settle(2)
    settle(3)
    normalise(2)
    normalise(3)
    relay(0)
    send_own(2)
    relay(1)
    send_own(3)
    relay_last(0)
    compute(0)
    relay(2)
    relay_last(1)
    both_halves(first_hop, 0)
    compute(1)
    relay(3)
    relay_last(2)
    both_halves(first_hop, 1)
    compute(2)
    both_halves(second_hop, 0)
    relay_last(3)
    both_halves(first_hop, 2)
    compute(3)
    both_halves(second_hop, 1)
    both_halves(first_hop, 3)
    both_halves(second_hop, 2)
    both_halves(finish, 0)
    both_halves(finish, 1)
    both_halves(second_hop, 3)
    both_halves(finish, 2)
    both_halves(finish, 3)
    @pl.when(row == 0)
    def sent_keys():
        arrive(rows.at[0], far_sem.at[0])

    @pl.when(row == 1)
    def sent_wide_queries():
        arrive(key_wide, wide_send.at[0])

    @pl.when(column == 1)
    def sent_slim_queries():
        arrive(key_slim, slim_send.at[0])

    @pl.when(column == 0)
    def sent_slim_replies():
        arrive(reply_slim, reply_send.at[1])
        arrive(denom_out.at[1], denom_send.at[1])

    arrive(info.at[:3], info_sem.at[2])
    arrive(key_slim, pair_send.at[1])
    arrive(reply_wide, reply_send.at[0])
    arrive(denom_out.at[0], denom_send.at[0])
    for whole, flag in (
        (info.at[:4], info_sem),
        (key_wide, pair_send),
        (mixed, mixed_send),
        (rows.at[:, part:, :], gather_send),
        (core_out, core_send),
        (hop_out, hop_send),
        (last_out, last_send),
    ):
        arrive(whole, flag.at[0])


def fused_block(*operands):
    queries, gates, gate_weight = operands[0], operands[4], operands[10]
    tokens, model_width = queries.shape
    devices = gates.shape[0]
    head_dim = model_width // devices
    hidden_width = gate_weight.shape[0]
    part = tokens // CHUNKS
    width = model_width // HALVES
    batch = devices * part
    near = pl.BlockSpec(memory_space=pltpu.VMEM)
    far = pl.BlockSpec(memory_space=pl.ANY)

    def space(*shape, kind=jnp.bfloat16):
        return pltpu.VMEM(shape, kind)

    def flags(*shape):
        return [pltpu.SemaphoreType.DMA((1,)), pltpu.SemaphoreType.DMA(shape)]

    return pl.pallas_call(
        fused_kernel,
        out_shape=pltpu.VMEM((tokens, model_width), jnp.bfloat16),
        in_specs=[far] * 13,
        out_specs=near,
        scratch_shapes=[
            space(devices, tokens, kind=jnp.float32),
            space(devices, tokens, kind=jnp.float32),
            space(2, tokens, kind=jnp.int32),
            space(2, tokens, kind=jnp.float32),
            space(1, model_width, kind=jnp.float32),
            space(1, model_width, kind=jnp.float32),
            space(devices, 24, tokens, kind=jnp.float32),
            space(devices, devices, tokens, kind=jnp.float32),
            space(devices, devices, tokens, kind=jnp.float32),
            space(4, 1, 4 * tokens, kind=jnp.float32),
            space(CHUNKS, 4 * part, 4, kind=jnp.float32),
            space(CHUNKS, batch, 1, kind=jnp.float32),
            space(CHUNKS, 4 * part, 2 * head_dim),
            space(CHUNKS, 4 * part, 2 * head_dim),
            space(4 * tokens, 2 * head_dim),
            space(4 * tokens, 2 * head_dim),
            space(2 * tokens, 2 * head_dim),
            space(2 * tokens, 2 * head_dim),
        ]
        + [space(CHUNKS, 2 * part, 2 * head_dim)] * 5
        + [
            space(CHUNKS, 2 * part, 4, kind=jnp.float32),
            space(2, CHUNKS, 2, tokens, kind=jnp.float32),
            space(3, CHUNKS, 2, tokens, kind=jnp.float32),
            space(CHUNKS, part, 4 * head_dim),
            space(CHUNKS, part, model_width),
            space(tokens, model_width),
            space(CHUNKS, batch, model_width),
            space(*gate_weight.shape),
            space(*gate_weight.shape),
            space(*gate_weight.shape),
            space(batch, hidden_width, kind=jnp.float32),
            space(batch, hidden_width, kind=jnp.float32),
            space(batch, hidden_width),
            space(2, HALVES, batch // 2, width),
            space(CHUNKS, HALVES, batch // 2, width),
            space(CHUNKS, HALVES, batch // 2, width),
            space(CHUNKS, HALVES, 2, part, width),
            space(CHUNKS, HALVES, 2, part, width),
            space(CHUNKS, HALVES, 2, part, width, kind=jnp.float32),
            space(CHUNKS, HALVES, part, width),
            space(CHUNKS, HALVES, part, width),
            pltpu.SemaphoreType.DMA((14 + 2 * CHUNKS,)),
            pltpu.SemaphoreType.DMA((4,)),
            pltpu.SemaphoreType.DMA((2,)),
            pltpu.SemaphoreType.DMA((CHUNKS + 1,)),
            pltpu.SemaphoreType.DMA((2,)),
        ]
        + flags(CHUNKS)
        + flags(CHUNKS)
        + [pltpu.SemaphoreType.DMA((2,)), pltpu.SemaphoreType.DMA((3, CHUNKS))] * 2
        + flags(CHUNKS)
        + flags(CHUNKS, 10)
        + flags(CHUNKS, HALVES)
        + flags(CHUNKS, HALVES, 2)
        + flags(CHUNKS, HALVES),
        compiler_params=pltpu.CompilerParams(
            collective_id=1, has_side_effects=True, vmem_limit_bytes=VMEM_BYTES
        ),
    )(*operands)


def shards(
    queries,
    key_vectors,
    value_vectors,
    residual_in,
    input_logit,
    forget_logit,
    mix_gain,
    ffn_gain,
    expert_gate,
    expert_up,
    expert_down,
    routes,
    route_weight,
):
    tokens, model_width = queries.shape
    head_count = input_logit.shape[0]
    head_dim = model_width // head_count
    devices = lax.axis_size("seq")
    group = devices // head_count
    group_width = model_width // devices
    if devices == 8 and head_count == 8:
        return fused_block(
            queries,
            key_vectors,
            value_vectors,
            residual_in,
            input_logit,
            forget_logit,
            jnp.transpose(routes),
            jnp.transpose(route_weight),
            mix_gain.reshape(1, -1),
            ffn_gain.reshape(1, -1),
            jnp.transpose(expert_gate[0]),
            jnp.transpose(expert_up[0]),
            expert_down[0],
        )

    capacity = 4 * tokens // devices
    flat_routes = routes.reshape(-1)
    matches = (flat_routes[:, None] == jnp.arange(devices, dtype=jnp.int32)[None, :]).astype(
        jnp.int32
    )
    before = jnp.cumsum(matches, axis=0) - matches
    position = jnp.sum(before * matches, axis=1)
    position = position.reshape(tokens, 2)
    slot_index = (flat_routes * capacity + position.reshape(-1)).reshape(tokens, 2)
    notes = jnp.stack(
        (jnp.repeat(input_logit, group, axis=0), jnp.repeat(forget_logit, group, axis=0)), axis=1
    )
    def columns_of(width, share):
        return lambda ref, other: ref.at[
            :, pl.ds(pl.multiple_of((other // share) * width, width), width)
        ]

    def rows_from(ref, origin):
        return ref.at[pl.ds(pl.multiple_of(origin * tokens, tokens), tokens), :]

    def entry(ref, other):
        return ref.at[other]

    head_columns = columns_of(head_dim, group)
    own_columns = columns_of(group_width, 1)
    tall = devices * tokens
    told, key_all, query_all, value_all = exchange(
        (
            (entry, entry),
            (head_columns, rows_from),
            (head_columns, rows_from),
            (own_columns, rows_from),
        ),
        devices,
        2,
        (notes, key_vectors, queries, value_vectors),
        (
            jax.ShapeDtypeStruct(notes.shape, jnp.float32),
            jax.ShapeDtypeStruct((tall, head_dim), jnp.bfloat16),
            jax.ShapeDtypeStruct((tall, head_dim), jnp.bfloat16),
            jax.ShapeDtypeStruct((tall, group_width), jnp.bfloat16),
        ),
    )
    mixed = head_mix(
        query_all, key_all, value_all, told[:, 0].reshape(-1), told[:, 1].reshape(-1)
    ).astype(jnp.bfloat16)
    (mixer_out,) = exchange(
        ((rows_from, own_columns),),
        devices,
        3,
        (mixed,),
        (jax.ShapeDtypeStruct((tokens, model_width), jnp.bfloat16),),
    )
    mixer_out = mixer_out.astype(jnp.float32)
    mixer_square = jnp.mean(mixer_out * mixer_out, axis=1, keepdims=True)
    updated = (
        residual_in.astype(jnp.float32) + mixer_out * lax.rsqrt(mixer_square + EPSILON) * mix_gain
    ).astype(jnp.bfloat16)
    updated_float = updated.astype(jnp.float32)
    updated_square = jnp.mean(updated_float * updated_float, axis=1, keepdims=True)
    normed = (updated_float * lax.rsqrt(updated_square + EPSILON) * ffn_gain).astype(jnp.bfloat16)
    columns = jnp.arange(devices * capacity, dtype=jnp.int32)
    pick_first = (slot_index[:, 0:1] == columns[None, :]).astype(jnp.bfloat16)
    pick_second = (slot_index[:, 1:2] == columns[None, :]).astype(jnp.bfloat16)
    spread = jnp.einsum(
        "tc,td->cd", pick_first + pick_second, normed, preferred_element_type=jnp.float32
    ).astype(jnp.bfloat16)
    outbound = spread.reshape(devices, capacity, model_width)
    block_in = lax.all_to_all(outbound, "seq", split_axis=0, concat_axis=0, tiled=True)
    row_block = block_in.reshape(-1, model_width)
    gate_val = jnp.dot(row_block, expert_gate[0], preferred_element_type=jnp.float32)
    up_val = jnp.dot(row_block, expert_up[0], preferred_element_type=jnp.float32)
    hidden = (jax.nn.silu(gate_val) * up_val).astype(jnp.bfloat16)
    result = jnp.dot(hidden, expert_down[0], preferred_element_type=jnp.float32).astype(
        jnp.bfloat16
    )
    inbound = lax.all_to_all(
        result.reshape(block_in.shape), "seq", split_axis=0, concat_axis=0, tiled=True
    )
    flat_back = inbound.reshape(devices * capacity, model_width)
    first_out = jnp.dot(pick_first, flat_back, preferred_element_type=jnp.float32)
    second_out = jnp.dot(pick_second, flat_back, preferred_element_type=jnp.float32)
    expert_mix = route_weight[:, 0:1] * first_out + route_weight[:, 1:2] * second_out
    return (updated_float + expert_mix).astype(jnp.bfloat16)


def solution(mesh):
    return jax.shard_map(
        shards,
        mesh=mesh,
        in_specs=(
            P(("batch", "seq"), None),
            P(("batch", "seq"), None),
            P(("batch", "seq"), None),
            P(("batch", "seq"), None),
            P(None, ("batch", "seq")),
            P(None, ("batch", "seq")),
            P(),
            P(),
            P("seq", None, None),
            P("seq", None, None),
            P("seq", None, None),
            P(("batch", "seq"), None),
            P(("batch", "seq"), None),
        ),
        out_specs=P(("batch", "seq"), None),
        check_vma=False,
    )
```

```python
import functools
import math

import jax
import jax.numpy as jnp
from jax import lax
from jax.experimental import pallas as pl
from jax.experimental.pallas import tpu as pltpu
from jax.sharding import PartitionSpec as P

EPSILON = 1e-06
CHUNKS = 4
HALVES = 2
FLIPS = (6, 4, 2, 7, 5, 3, 1)
SLOT_ORDER = (0, 2, 4, 6, 1, 3, 5, 7)
VMEM_BYTES = 64 * 1024 * 1024 - 1280 * 1024
LOW = -1e30


def exchange_kernel(moves, devices, *refs):
    count = len(moves)
    sources, targets = refs[:count], refs[count : 2 * count]
    send_sem, recv_sem, local_sem = refs[2 * count :]
    me = lax.axis_index("seq")
    others = [lax.rem(me + step, devices) for step in range(1, devices)]
    barrier = pltpu.get_barrier_semaphore()
    for other in others:
        pl.semaphore_signal(
            barrier, inc=1, device_id={"seq": other}, device_id_type=pl.DeviceIdType.MESH
        )
    pl.semaphore_wait(barrier, devices - 1)
    copies = []
    for i, (take, put) in enumerate(moves):
        for step, other in enumerate(others):
            copies.append(
                pltpu.make_async_remote_copy(
                    src_ref=take(sources[i], other),
                    dst_ref=put(targets[i], me),
                    send_sem=send_sem.at[i, step],
                    recv_sem=recv_sem.at[i, step],
                    device_id={"seq": other},
                    device_id_type=pl.DeviceIdType.MESH,
                )
            )
            copies[-1].start()
    for i, (take, put) in enumerate(moves):
        copies.append(
            pltpu.make_async_copy(take(sources[i], me), put(targets[i], me), local_sem.at[i])
        )
        copies[-1].start()
    for copy in copies:
        copy.wait()


def exchange(moves, devices, number, sources, shapes):
    far = pl.BlockSpec(memory_space=pl.ANY)
    count = len(moves)
    return pl.pallas_call(
        functools.partial(exchange_kernel, moves, devices),
        out_shape=shapes,
        in_specs=[far] * count,
        out_specs=[far] * count,
        scratch_shapes=[
            pltpu.SemaphoreType.DMA((count, devices - 1)),
            pltpu.SemaphoreType.DMA((count, devices - 1)),
            pltpu.SemaphoreType.DMA((count,)),
        ],
        compiler_params=pltpu.CompilerParams(collective_id=number, has_side_effects=True),
    )(*sources)


def head_mix(query, key, value, input_gate, forget_gate):
    positions, head_dim = query.shape
    cumul_log = jnp.cumsum(jax.nn.log_sigmoid(forget_gate))
    level = input_gate - cumul_log
    top = lax.cummax(level, axis=0)
    scores = lax.dot_general(
        query, key, (((1,), (1,)), ((), ())), preferred_element_type=jnp.float32
    )
    causal = jnp.arange(positions)[:, None] >= jnp.arange(positions)[None, :]
    decay = jnp.exp(jnp.minimum(level[None, :] - top[:, None], 0.0))
    coef = jnp.where(causal, decay * scores, 0.0) * (1.0 / math.sqrt(head_dim))
    denom_sum = jnp.sum(coef, axis=1, keepdims=True)
    numer_sum = jnp.dot(coef.astype(jnp.bfloat16), value, preferred_element_type=jnp.float32)
    return numer_sum / jnp.maximum(jnp.abs(denom_sum), 1.0)


def fused_kernel(
    query_far,
    key_far,
    value_far,
    residual_far,
    input_far,
    forget_far,
    routes_far,
    weights_far,
    mix_far,
    ffn_far,
    gate_far,
    up_far,
    down_far,
    out,
    input_gate,
    forget_gate,
    routes,
    weights,
    mix_gain,
    ffn_gain,
    info,
    level,
    peak_before,
    key_level,
    top,
    slot_weight,
    query_wide,
    query_slim,
    key_wide,
    value_wide,
    key_slim,
    value_slim,
    reply_wide,
    reply_slim,
    from_far_row,
    from_near_wide,
    from_near_slim,
    denom,
    denom_out,
    denom_in,
    mixed,
    mixer_in,
    updated,
    rows,
    gate,
    up,
    down,
    gate_sum,
    up_sum,
    hidden,
    own,
    core_out,
    core_in,
    hop_out,
    hop_in,
    keep,
    last_out,
    last_in,
    load_sem,
    info_sem,
    pair_send,
    pair_recv,
    far_sem,
    wide_send,
    wide_recv,
    slim_send,
    slim_recv,
    reply_send,
    reply_recv,
    denom_send,
    denom_recv,
    mixed_send,
    mixed_recv,
    gather_send,
    gather_recv,
    core_send,
    core_recv,
    hop_send,
    hop_recv,
    last_send,
    last_recv,
):
    me = lax.axis_index("seq")
    heads, tokens = input_gate.shape
    devices = heads
    model_width = out.shape[1]
    head_dim = model_width // heads
    part = tokens // CHUNKS
    width = model_width // HALVES
    four = devices // 2 * part
    slice_width = 2 * head_dim
    core = lax.rem(me, 2)
    column = lax.rem(lax.div(me, 2), 2)
    row = lax.div(me, 4)
    chip = lax.div(me, 2)
    chip_x = chip + 1 - 2 * column
    chip_y = chip + 2 - 4 * row
    key_chip = chip_x * (1 - row) + chip_y * row
    query_chip = chip_y * (1 - row) + chip_x * row
    wide_base = (1 - row) * width
    slim_base = row * width
    bases = (wide_base, slim_base)

    def peer(flip):
        total = 0
        for bit in (1, 2, 4):
            own_bit = lax.rem(lax.div(me, bit), 2)
            total = total + bit * ((1 - own_bit) if flip & bit else own_bit)
        return total

    def arrive(whole, flag):
        pltpu.make_async_copy(whole, whole, flag).wait()

    def prepared(source, target, send_sem, recv_sem, flip):
        return pltpu.make_async_remote_copy(
            src_ref=source,
            dst_ref=target,
            send_sem=send_sem,
            recv_sem=recv_sem,
            device_id={"seq": peer(flip)},
            device_id_type=pl.DeviceIdType.MESH,
        )

    def remote(*arguments):
        copy = prepared(*arguments)
        copy.start()
        return copy

    def span_of(index, count, first=0):
        return pl.ds(pl.multiple_of(index * count + first, count), count)

    def head_columns(base, owner):
        return pl.ds(pl.multiple_of(base + owner * slice_width, slice_width), slice_width)

    def core_of(flip):
        return 1 - core if flip % 2 else core

    barrier = pltpu.get_barrier_semaphore()
    for flip in FLIPS:
        pl.semaphore_signal(
            barrier,
            inc=1,
            device_id={"seq": peer(flip)},
            device_id_type=pl.DeviceIdType.MESH,
        )
    small = (
        (input_far, input_gate),
        (forget_far, forget_gate),
        (routes_far, routes),
        (weights_far, weights),
        (mix_far, mix_gain),
        (ffn_far, ffn_gain),
    )
    blocks = tuple(
        (far.at[:, head_columns(base, core)], target.at[span_of(core, tokens), :])
        for base, far, target in (
            (wide_base, key_far, key_wide),
            (wide_base, value_far, value_wide),
            (slim_base, key_far, key_slim),
            (slim_base, value_far, value_slim),
        )
    ) + tuple(
        (
            query_far.at[pl.ds(j * part, part), head_columns(base, core)],
            target.at[j, span_of(core, part), :],
        )
        for j in range(CHUNKS)
        for base, target in ((wide_base, query_wide), (slim_base, query_slim))
    )
    large = ((residual_far, updated), (gate_far, gate), (up_far, up), (down_far, down))
    loads = [
        pltpu.make_async_copy(source, target, load_sem.at[i])
        for i, (source, target) in enumerate(small + blocks + large)
    ]
    small_loads, block_loads, large_loads = loads[:6], loads[6:18], loads[18:]
    for load in small_loads + block_loads:
        load.start()
    for load in small_loads:
        load.wait()
    forget = forget_gate[...]
    info[me, 0:8, :] = input_gate[...]
    info[me, 8:16, :] = -(jnp.maximum(-forget, 0.0) + jnp.log1p(jnp.exp(-jnp.abs(forget))))
    info[me, 16:18, :] = routes[...].astype(jnp.float32)
    info[me, 18:20, :] = weights[...]
    pl.semaphore_wait(barrier, devices - 1)

    for flip in (6, 4, 2, 1):
        remote(info.at[me], info.at[me], info_sem.at[0], info_sem.at[1], flip)

    @pl.when(row == 0)
    def send_keys():
        for i in range(2):
            for far, target in ((key_far, key_wide), (value_far, value_wide)):
                for flip, base in ((2, wide_base), (4, slim_base), (3, wide_base), (5, slim_base)):
                    first = base + core_of(flip) * slice_width + i * head_dim
                    remote(
                        far.at[:, pl.ds(pl.multiple_of(first, head_dim), head_dim)],
                        target.at[
                            span_of(core, tokens, 2 * tokens), pl.ds(i * head_dim, head_dim)
                        ],
                        far_sem.at[0],
                        far_sem.at[1 + i],
                        flip,
                    )

    @pl.when(column == 1)
    def send_slim_queries():
        for j in range(CHUNKS):
            for flip in (2, 3):
                remote(
                    query_far.at[pl.ds(j * part, part), head_columns(slim_base, core_of(flip))],
                    query_slim.at[j, span_of(core, part, 2 * part), :],
                    slim_send.at[0],
                    slim_recv.at[j],
                    flip,
                )

    @pl.when(row == 1)
    def send_wide_queries():
        for j in range(CHUNKS):
            for flip, base in ((2, wide_base), (4, slim_base), (3, wide_base), (5, slim_base)):
                remote(
                    query_far.at[pl.ds(j * part, part), head_columns(base, core_of(flip))],
                    query_wide.at[j, span_of(core, part, 2 * part), :],
                    wide_send.at[0],
                    wide_recv.at[j],
                    flip,
                )

    for base, far, target in (
        (wide_base, key_far, key_wide),
        (wide_base, value_far, value_wide),
        (slim_base, key_far, key_slim),
        (slim_base, value_far, value_slim),
    ):
        remote(
            far.at[:, head_columns(base, 1 - core)],
            target.at[span_of(core, tokens), :],
            pair_send.at[0],
            pair_recv.at[CHUNKS],
            1,
        )
    for j in range(CHUNKS):
        for base, target in ((wide_base, query_wide), (slim_base, query_slim)):
            remote(
                query_far.at[pl.ds(j * part, part), head_columns(base, 1 - core)],
                target.at[j, span_of(core, part), :],
                pair_send.at[1],
                pair_recv.at[j],
                1,
            )
    for load in large_loads:
        load.start()

    arrive(info.at[:4], info_sem.at[1])
    for flip in (2, 4, 6):
        told = info.at[peer(flip)]
        remote(told, told, info_sem.at[2], info_sem.at[3], 1)
    arrive(info.at[:3], info_sem.at[3])
    across = lax.broadcasted_iota(jnp.int32, (tokens, tokens), 0)
    along = lax.broadcasted_iota(jnp.int32, (tokens, tokens), 1)
    local_sum = jnp.dot(
        info[:, 8:16, :].reshape(devices * heads, tokens),
        (across <= along).astype(jnp.float32),
        precision=lax.Precision.HIGHEST,
        preferred_element_type=jnp.float32,
    )
    before = jnp.zeros((heads, 1), jnp.float32)
    peak = jnp.full((heads, 1), LOW, jnp.float32)
    for block in range(devices):
        lines = local_sum[block * heads : (block + 1) * heads, :]
        level_lines = info[block, 0:8, :] - (lines + before)
        before = before + lines[:, tokens - 1 : tokens]
        level[block] = level_lines
        peak_before[block] = jnp.broadcast_to(peak, (heads, tokens))
        peak = jnp.maximum(peak, jnp.max(level_lines, axis=1, keepdims=True))
    for group, first_chip in ((0, query_chip), (1, chip_x)):
        for i in range(2):
            head = (row if group else 1 - row) * (heads // 2) + 2 * core + i
            for slot in range(4):
                block = 2 * (chip if slot < 2 else first_chip) + slot % 2
                line = level[block, pl.ds(head, 1), :]
                if slot < 2:
                    key_level[2 * group + i, :, slot * tokens : (slot + 1) * tokens] = line
                spread = jnp.where(along <= across, jnp.broadcast_to(line, (tokens, tokens)), LOW)
                tops = jnp.maximum(
                    jnp.max(spread, axis=1, keepdims=True),
                    peak_before[block, pl.ds(head, 1), :][:, 0:1],
                )
                for j in range(CHUNKS):
                    top[j, slot * part : (slot + 1) * part, 2 * group + i : 2 * group + i + 1] = (
                        tops[j * part : (j + 1) * part, :]
                    )
            if group == 0:
                for slot in (2, 3):
                    key_level[i, :, slot * tokens : (slot + 1) * tokens] = level[
                        2 * key_chip + slot % 2, pl.ds(head, 1), :
                    ]

    query_row = lax.broadcasted_iota(jnp.int32, (4 * part, 1), 0)
    row_block = lax.shift_right_logical(query_row, part.bit_length() - 1)
    foreign_row = row_block >= 2
    row_place = (
        jnp.where(foreign_row, row_block - 2, row_block) * (tokens - part)
        + query_row
        - jnp.where(foreign_row, 2 * part, 0)
    )
    diagonal = across[: 2 * part, :] == along[: 2 * part, :]
    key_lane = lax.broadcasted_iota(jnp.int32, (1, 4 * tokens), 1)
    wide_place = jnp.where(
        key_lane < 2 * tokens,
        chip * (2 * tokens) + key_lane,
        key_chip * (2 * tokens) + key_lane - 2 * tokens,
    )

    def attend(j, group, query, key, value, key_place, foreign_chip, reply, parts):
        place = row_place + j * part + jnp.where(foreign_row, foreign_chip, chip) * (2 * tokens)
        causal = key_place <= place
        keys = key.shape[0]
        for i in parts:
            number = 2 * group + i
            view = slice(i * head_dim, (i + 1) * head_dim)
            scores = lax.dot_general(
                query[j, :, view],
                key[:, view],
                (((1,), (1,)), ((), ())),
                preferred_element_type=jnp.float32,
            )
            decay = jnp.exp(
                jnp.minimum(key_level[number, :, 0:keys] - top[j, :, number : number + 1], 0.0)
            )
            coef = jnp.where(causal, decay * scores, 0.0) * (1.0 / math.sqrt(head_dim))
            denom_sum = jnp.sum(coef, axis=1, keepdims=True)
            numer_sum = jnp.dot(
                coef.astype(jnp.bfloat16), value[:, view], preferred_element_type=jnp.float32
            )
            for slot in range(2):
                keep[j, group, i, :, slot * head_dim : (slot + 1) * head_dim] = numer_sum[
                    slot * part : (slot + 1) * part, :
                ]
            denom[j, :, number : number + 1] = denom_sum[: 2 * part, :]
            reply[j, :, view] = numer_sum[2 * part :, :].astype(jnp.bfloat16)
            denom_out[group, j, i : i + 1, :] = jnp.sum(
                jnp.where(diagonal, denom_sum[2 * part :, :], 0.0), axis=0, keepdims=True
            )

    def answer(j, group, number, reply, target, flip, view, flag):
        remote(
            reply.at[j, :, view],
            target.at[j, :, view],
            reply_send.at[group],
            reply_recv.at[flag, j],
            flip,
        )
        if flag == number:
            remote(
                denom_out.at[group, j],
                denom_in.at[number, j],
                denom_send.at[group],
                denom_recv.at[number, j],
                flip,
            )

    def attend_slim(j):
        @pl.when(column == 0)
        def receive():
            arrive(query_slim.at[j, 2 * part :, :], slim_recv.at[j])

        attend(
            j,
            1,
            query_slim,
            key_slim,
            value_slim,
            chip * (2 * tokens) + key_lane[:, : 2 * tokens],
            chip_x,
            reply_slim,
            (0, 1),
        )

        @pl.when(column == 0)
        def answer_slim():
            answer(j, 1, 0, reply_slim, from_near_slim, 2, pl.ds(0, slice_width), 0)

    def attend_wide(j, i):
        if i == 0:
            arrive(query_wide.at[j, 2 * part :, :], wide_recv.at[j])
        attend(j, 0, query_wide, key_wide, value_wide, wide_place, query_chip, reply_wide, (i,))
        view = pl.ds(i * head_dim, head_dim)

        @pl.when(row == 0)
        def answer_far():
            answer(j, 0, 1, reply_wide, from_far_row, 4, view, 3 - 2 * i)

        @pl.when(row == 1)
        def answer_near():
            answer(j, 0, 2, reply_wide, from_near_wide, 2, view, 4 - 2 * i)

    def add_reply(j, group, number, source):
        if number == 0:
            arrive(source.at[j], reply_recv.at[number, j])
        else:
            arrive(source.at[j, :, :head_dim], reply_recv.at[number + 2, j])
            arrive(source.at[j, :, head_dim:], reply_recv.at[number, j])
        arrive(denom_in.at[number, j], denom_recv.at[number, j])
        for i in range(2):
            for slot in range(2):
                view = slice(slot * head_dim, (slot + 1) * head_dim)
                keep[j, group, i, :, view] += source[
                    j, slot * part : (slot + 1) * part, i * head_dim : (i + 1) * head_dim
                ].astype(jnp.float32)
            place = 2 * group + i
            denom[j, :, place : place + 1] += jnp.sum(
                jnp.where(diagonal, denom_in[number, j, i : i + 1, :], 0.0),
                axis=1,
                keepdims=True,
            )

    def settle(j):
        @pl.when(row == 1)
        def add_row():
            add_reply(j, 1, 1, from_far_row)
            add_reply(j, 0, 2, from_near_wide)

        @pl.when(column == 1)
        def add_column():
            add_reply(j, 1, 0, from_near_slim)

        for group in range(2):
            for i in range(2):
                number = 2 * group + i
                for owner in (core, 1 - core):
                    divisor = denom[j, span_of(owner, part), :][:, number : number + 1]
                    value = (
                        keep[j, group, i, :, span_of(owner, head_dim)]
                        / jnp.maximum(jnp.abs(divisor), 1.0)
                    ).astype(jnp.bfloat16)
                    if owner is core:
                        first = bases[group] + core * slice_width + i * head_dim
                        mixer_in[j, :, pl.ds(pl.multiple_of(first, head_dim), head_dim)] = value
                    else:
                        first = group * slice_width + i * head_dim
                        mixed[j, :, first : first + head_dim] = value
            remote(
                mixed.at[j, :, pl.ds(group * slice_width, slice_width)],
                mixer_in.at[j, :, head_columns(bases[group], core)],
                mixed_send.at[0],
                mixed_recv.at[j],
                1,
            )

    def weigh():
        for slot in range(devices):
            told = info.at[peer(slot)] if slot else info.at[me]
            line = jnp.where(
                told[16:17, :].astype(jnp.int32) == me, told[18:19, :], 0.0
            ) + jnp.where(told[17:18, :].astype(jnp.int32) == me, told[19:20, :], 0.0)
            spread = jnp.where(along == across, jnp.broadcast_to(line, (tokens, tokens)), 0.0)
            weight_column = jnp.sum(spread, axis=1, keepdims=True)
            place = SLOT_ORDER.index(slot) * part
            for j in range(CHUNKS):
                slot_weight[j, place : place + part, :] = weight_column[
                    j * part : (j + 1) * part, :
                ]

    def slot_rows(slot):
        return pl.ds(SLOT_ORDER.index(slot) * part, part)

    def columns(half):
        return pl.ds(half * width, width)

    gathers = {}

    def gather(j, number, source, target, flip, half=None, begin=remote):
        view = slice(None) if half is None else columns(half)
        gathers[j, number] = begin(
            rows.at[j, slot_rows(source), view],
            rows.at[j, slot_rows(target), view],
            gather_send.at[0],
            gather_recv.at[j, number],
            flip,
        )

    def normalise(j):
        arrive(mixed.at[j], mixed_recv.at[j])
        if j == 0:
            large_loads[0].wait()
        span = slice(j * part, (j + 1) * part)
        mixer_out = mixer_in[j].astype(jnp.float32)
        square = jnp.mean(mixer_out * mixer_out, axis=1, keepdims=True)
        value = (
            updated[span, :].astype(jnp.float32)
            + mixer_out * lax.rsqrt(square + EPSILON) * mix_gain[...]
        ).astype(jnp.bfloat16)
        updated[span, :] = value
        value = value.astype(jnp.float32)
        square = jnp.mean(value * value, axis=1, keepdims=True)
        rows[j, 0:part, :] = (value * lax.rsqrt(square + EPSILON) * ffn_gain[...]).astype(
            jnp.bfloat16
        )

    def send_own(j, begin=remote):
        gather(j, 0, 0, 2, 2, 0, begin)
        gather(j, 1, 0, 4, 4, 1, begin)
        gather(j, 2, 0, 2, 2, 1, begin)
        gather(j, 3, 0, 4, 4, 0, begin)
        gather(j, 4, 0, 1, 1, None, begin)

    def attend_first():
        place = row_place[: 2 * part, :] + chip * (2 * tokens)
        causal = key_lane[:, : 2 * tokens] + chip * (2 * tokens) <= place
        for group, query, key, value in (
            (0, query_wide, key_wide, value_wide),
            (1, query_slim, key_slim, value_slim),
        ):
            for i in range(2):
                number = 2 * group + i
                view = slice(i * head_dim, (i + 1) * head_dim)
                scores = lax.dot_general(
                    query[0, : 2 * part, view],
                    key[: 2 * tokens, view],
                    (((1,), (1,)), ((), ())),
                    preferred_element_type=jnp.float32,
                )
                decay = jnp.exp(
                    jnp.minimum(
                        key_level[number, :, : 2 * tokens]
                        - top[0, : 2 * part, number : number + 1],
                        0.0,
                    )
                )
                coef = jnp.where(causal, decay * scores, 0.0) * (1.0 / math.sqrt(head_dim))
                denom[0, :, number : number + 1] = jnp.sum(coef, axis=1, keepdims=True)
                numer_sum = jnp.dot(
                    coef.astype(jnp.bfloat16),
                    value[: 2 * tokens, view],
                    preferred_element_type=jnp.float32,
                )
                for slot in range(2):
                    keep[0, group, i, :, slot * head_dim : (slot + 1) * head_dim] = numer_sum[
                        slot * part : (slot + 1) * part, :
                    ]

    def open_first():
        settle(0)
        normalise(0)
        for number in (0, 1, 2):
            gathers[0, number].start()

    def relay(j):
        gathers[j, 0].wait_recv()
        gather(j, 5, 2, 6, 4, 0)
        gathers[j, 1].wait_recv()
        gather(j, 6, 4, 6, 2, 1)
        gathers[j, 2].wait_recv()
        gather(j, 7, 2, 3, 1)
        gathers[j, 3].wait_recv()
        gather(j, 8, 4, 5, 1)

    def relay_last(j):
        gathers[j, 5].wait_recv()
        gathers[j, 6].wait_recv()
        gather(j, 9, 6, 7, 1)

    core_copies, hop_copies, last_copies = {}, {}, {}

    def compute(j):
        for number in (4, 7, 8, 9):
            gathers[j, number].wait_recv()
        if j == 0:
            large_loads[1].wait()
            large_loads[2].wait()
        for weight, total in ((gate, gate_sum), (up, up_sum)):
            total[...] = lax.dot_general(
                rows[j],
                weight[...],
                (((1,), (1,)), ((), ())),
                preferred_element_type=jnp.float32,
            )
        gate_val = gate_sum[...]
        hidden[...] = (gate_val / (1.0 + jnp.exp(-gate_val)) * up_sum[...]).astype(jnp.bfloat16)
        if j == 0:
            large_loads[3].wait()
        for half in range(HALVES):
            terms = (
                jnp.dot(hidden[...], down[:, columns(half)], preferred_element_type=jnp.float32)
                * slot_weight[j]
            ).astype(jnp.bfloat16)
            own[j % 2, half] = terms[:four, :]
            core_out[j, half] = terms[four:, :]
            core_copies[j, half] = remote(
                core_out.at[j, half],
                core_in.at[j, half],
                core_send.at[0],
                core_recv.at[j, half],
                1,
            )

    def first_hop(j, half):
        first, second = (2, 4) if half == 0 else (4, 2)
        core_copies[j, half].wait_recv()
        for slot in (6, first, second, 0):
            view = slot_rows(slot)
            both = own[j % 2, half, view, :].astype(jnp.float32) + core_in[
                j, half, view, :
            ].astype(jnp.float32)
            if slot in (0, second):
                keep[j, half, 0 if slot == 0 else 1] = both
                continue
            place = 1 if slot == 6 else 0
            hop_out[j, half, place] = both.astype(jnp.bfloat16)
            hop_copies[j, half, place] = remote(
                hop_out.at[j, half, place],
                hop_in.at[j, half, place],
                hop_send.at[0],
                hop_recv.at[j, half, place],
                first,
            )

    def second_hop(j, half):
        second = 4 if half == 0 else 2
        hop_copies[j, half, 1].wait_recv()
        last_out[j, half] = (
            keep[j, half, 1] + hop_in[j, half, 1].astype(jnp.float32)
        ).astype(jnp.bfloat16)
        last_copies[j, half] = remote(
            last_out.at[j, half],
            last_in.at[j, half],
            last_send.at[0],
            last_recv.at[j, half],
            second,
        )

    def finish(j, half):
        hop_copies[j, half, 0].wait_recv()
        last_copies[j, half].wait_recv()
        span = slice(j * part, (j + 1) * part)
        out[span, columns(half)] = (
            updated[span, columns(half)].astype(jnp.float32)
            + (
                keep[j, half, 0]
                + hop_in[j, half, 0].astype(jnp.float32)
                + last_in[j, half].astype(jnp.float32)
            )
        ).astype(jnp.bfloat16)

    def both_halves(step, j):
        for half in range(HALVES):
            step(j, half)

    arrive(key_wide, pair_recv.at[CHUNKS])
    for load in block_loads:
        load.wait()
    for j in range(CHUNKS):
        arrive(query_wide.at[j, : 2 * part, :], pair_recv.at[j])

    @pl.when(row == 1)
    def slim_early():
        for j in range(CHUNKS):
            attend_slim(j)

    send_own(0, prepared)

    @pl.when(chip == 0)
    def open_early():
        attend_first()
        open_first()

    weigh()
    arrive(key_slim, far_sem.at[1])
    for j in range(CHUNKS // 2):
        attend_wide(j, 0)
    arrive(key_slim, far_sem.at[2])
    attend_wide(0, 1)
    attend_wide(1, 1)

    @pl.when(row == 0)
    def slim_first():
        attend_slim(0)

    attend_wide(2, 0)
    attend_wide(2, 1)

    @pl.when(row == 0)
    def slim_second():
        attend_slim(1)

    attend_wide(3, 0)
    attend_wide(3, 1)

    @pl.when(row == 0)
    def slim_late():
        attend_slim(2)
        attend_slim(3)

    @pl.when(chip > 0)
    def open_late():
        open_first()

    gathers[0, 3].start()
    gathers[0, 4].start()
    settle(1)
    normalise(1)
    send_own(1)
    settle(2)
    settle(3)
    normalise(2)
    normalise(3)
    relay(0)
    send_own(2)
    relay(1)
    send_own(3)
    relay_last(0)
    compute(0)
    relay(2)
    relay_last(1)
    both_halves(first_hop, 0)
    compute(1)
    relay(3)
    relay_last(2)
    both_halves(first_hop, 1)
    compute(2)
    both_halves(second_hop, 0)
    relay_last(3)
    both_halves(first_hop, 2)
    compute(3)
    both_halves(second_hop, 1)
    both_halves(first_hop, 3)
    both_halves(second_hop, 2)
    both_halves(finish, 0)
    both_halves(finish, 1)
    both_halves(second_hop, 3)
    both_halves(finish, 2)
    both_halves(finish, 3)
    @pl.when(row == 0)
    def sent_keys():
        arrive(rows.at[0], far_sem.at[0])

    @pl.when(row == 1)
    def sent_wide_queries():
        arrive(key_wide, wide_send.at[0])

    @pl.when(column == 1)
    def sent_slim_queries():
        arrive(key_slim, slim_send.at[0])

    @pl.when(column == 0)
    def sent_slim_replies():
        arrive(reply_slim, reply_send.at[1])
        arrive(denom_out.at[1], denom_send.at[1])

    arrive(info.at[:3], info_sem.at[2])
    arrive(key_slim, pair_send.at[1])
    arrive(reply_wide, reply_send.at[0])
    arrive(denom_out.at[0], denom_send.at[0])
    for whole, flag in (
        (info.at[:4], info_sem),
        (key_wide, pair_send),
        (mixed, mixed_send),
        (rows.at[:, part:, :], gather_send),
        (core_out, core_send),
        (hop_out, hop_send),
        (last_out, last_send),
    ):
        arrive(whole, flag.at[0])


def fused_block(*operands):
    queries, gates, gate_weight = operands[0], operands[4], operands[10]
    tokens, model_width = queries.shape
    devices = gates.shape[0]
    head_dim = model_width // devices
    hidden_width = gate_weight.shape[0]
    part = tokens // CHUNKS
    width = model_width // HALVES
    batch = devices * part
    near = pl.BlockSpec(memory_space=pltpu.VMEM)
    far = pl.BlockSpec(memory_space=pl.ANY)

    def space(*shape, kind=jnp.bfloat16):
        return pltpu.VMEM(shape, kind)

    def flags(*shape):
        return [pltpu.SemaphoreType.DMA((1,)), pltpu.SemaphoreType.DMA(shape)]

    return pl.pallas_call(
        fused_kernel,
        out_shape=pltpu.VMEM((tokens, model_width), jnp.bfloat16),
        in_specs=[far] * 13,
        out_specs=near,
        scratch_shapes=[
            space(devices, tokens, kind=jnp.float32),
            space(devices, tokens, kind=jnp.float32),
            space(2, tokens, kind=jnp.int32),
            space(2, tokens, kind=jnp.float32),
            space(1, model_width, kind=jnp.float32),
            space(1, model_width, kind=jnp.float32),
            space(devices, 24, tokens, kind=jnp.float32),
            space(devices, devices, tokens, kind=jnp.float32),
            space(devices, devices, tokens, kind=jnp.float32),
            space(4, 1, 4 * tokens, kind=jnp.float32),
            space(CHUNKS, 4 * part, 4, kind=jnp.float32),
            space(CHUNKS, batch, 1, kind=jnp.float32),
            space(CHUNKS, 4 * part, 2 * head_dim),
            space(CHUNKS, 4 * part, 2 * head_dim),
            space(4 * tokens, 2 * head_dim),
            space(4 * tokens, 2 * head_dim),
            space(2 * tokens, 2 * head_dim),
            space(2 * tokens, 2 * head_dim),
        ]
        + [space(CHUNKS, 2 * part, 2 * head_dim)] * 5
        + [
            space(CHUNKS, 2 * part, 4, kind=jnp.float32),
            space(2, CHUNKS, 2, tokens, kind=jnp.float32),
            space(3, CHUNKS, 2, tokens, kind=jnp.float32),
            space(CHUNKS, part, 4 * head_dim),
            space(CHUNKS, part, model_width),
            space(tokens, model_width),
            space(CHUNKS, batch, model_width),
            space(*gate_weight.shape),
            space(*gate_weight.shape),
            space(*gate_weight.shape),
            space(batch, hidden_width, kind=jnp.float32),
            space(batch, hidden_width, kind=jnp.float32),
            space(batch, hidden_width),
            space(2, HALVES, batch // 2, width),
            space(CHUNKS, HALVES, batch // 2, width),
            space(CHUNKS, HALVES, batch // 2, width),
            space(CHUNKS, HALVES, 2, part, width),
            space(CHUNKS, HALVES, 2, part, width),
            space(CHUNKS, HALVES, 2, part, width, kind=jnp.float32),
            space(CHUNKS, HALVES, part, width),
            space(CHUNKS, HALVES, part, width),
            pltpu.SemaphoreType.DMA((14 + 2 * CHUNKS,)),
            pltpu.SemaphoreType.DMA((4,)),
            pltpu.SemaphoreType.DMA((2,)),
            pltpu.SemaphoreType.DMA((CHUNKS + 1,)),
            pltpu.SemaphoreType.DMA((3,)),
        ]
        + flags(CHUNKS)
        + flags(CHUNKS)
        + [pltpu.SemaphoreType.DMA((2,)), pltpu.SemaphoreType.DMA((5, CHUNKS))]
        + [pltpu.SemaphoreType.DMA((2,)), pltpu.SemaphoreType.DMA((3, CHUNKS))]
        + flags(CHUNKS)
        + flags(CHUNKS, 10)
        + flags(CHUNKS, HALVES)
        + flags(CHUNKS, HALVES, 2)
        + flags(CHUNKS, HALVES),
        compiler_params=pltpu.CompilerParams(
            collective_id=1, has_side_effects=True, vmem_limit_bytes=VMEM_BYTES
        ),
    )(*operands)


def shards(
    queries,
    key_vectors,
    value_vectors,
    residual_in,
    input_logit,
    forget_logit,
    mix_gain,
    ffn_gain,
    expert_gate,
    expert_up,
    expert_down,
    routes,
    route_weight,
):
    tokens, model_width = queries.shape
    head_count = input_logit.shape[0]
    head_dim = model_width // head_count
    devices = lax.axis_size("seq")
    group = devices // head_count
    group_width = model_width // devices
    if devices == 8 and head_count == 8:
        return fused_block(
            queries,
            key_vectors,
            value_vectors,
            residual_in,
            input_logit,
            forget_logit,
            jnp.transpose(routes),
            jnp.transpose(route_weight),
            mix_gain.reshape(1, -1),
            ffn_gain.reshape(1, -1),
            jnp.transpose(expert_gate[0]),
            jnp.transpose(expert_up[0]),
            expert_down[0],
        )

    capacity = 4 * tokens // devices
    flat_routes = routes.reshape(-1)
    matches = (flat_routes[:, None] == jnp.arange(devices, dtype=jnp.int32)[None, :]).astype(
        jnp.int32
    )
    before = jnp.cumsum(matches, axis=0) - matches
    position = jnp.sum(before * matches, axis=1)
    position = position.reshape(tokens, 2)
    slot_index = (flat_routes * capacity + position.reshape(-1)).reshape(tokens, 2)
    notes = jnp.stack(
        (jnp.repeat(input_logit, group, axis=0), jnp.repeat(forget_logit, group, axis=0)), axis=1
    )
    def columns_of(width, share):
        return lambda ref, other: ref.at[
            :, pl.ds(pl.multiple_of((other // share) * width, width), width)
        ]

    def rows_from(ref, origin):
        return ref.at[pl.ds(pl.multiple_of(origin * tokens, tokens), tokens), :]

    def entry(ref, other):
        return ref.at[other]

    head_columns = columns_of(head_dim, group)
    own_columns = columns_of(group_width, 1)
    tall = devices * tokens
    told, key_all, query_all, value_all = exchange(
        (
            (entry, entry),
            (head_columns, rows_from),
            (head_columns, rows_from),
            (own_columns, rows_from),
        ),
        devices,
        2,
        (notes, key_vectors, queries, value_vectors),
        (
            jax.ShapeDtypeStruct(notes.shape, jnp.float32),
            jax.ShapeDtypeStruct((tall, head_dim), jnp.bfloat16),
            jax.ShapeDtypeStruct((tall, head_dim), jnp.bfloat16),
            jax.ShapeDtypeStruct((tall, group_width), jnp.bfloat16),
        ),
    )
    mixed = head_mix(
        query_all, key_all, value_all, told[:, 0].reshape(-1), told[:, 1].reshape(-1)
    ).astype(jnp.bfloat16)
    (mixer_out,) = exchange(
        ((rows_from, own_columns),),
        devices,
        3,
        (mixed,),
        (jax.ShapeDtypeStruct((tokens, model_width), jnp.bfloat16),),
    )
    mixer_out = mixer_out.astype(jnp.float32)
    mixer_square = jnp.mean(mixer_out * mixer_out, axis=1, keepdims=True)
    updated = (
        residual_in.astype(jnp.float32) + mixer_out * lax.rsqrt(mixer_square + EPSILON) * mix_gain
    ).astype(jnp.bfloat16)
    updated_float = updated.astype(jnp.float32)
    updated_square = jnp.mean(updated_float * updated_float, axis=1, keepdims=True)
    normed = (updated_float * lax.rsqrt(updated_square + EPSILON) * ffn_gain).astype(jnp.bfloat16)
    columns = jnp.arange(devices * capacity, dtype=jnp.int32)
    pick_first = (slot_index[:, 0:1] == columns[None, :]).astype(jnp.bfloat16)
    pick_second = (slot_index[:, 1:2] == columns[None, :]).astype(jnp.bfloat16)
    spread = jnp.einsum(
        "tc,td->cd", pick_first + pick_second, normed, preferred_element_type=jnp.float32
    ).astype(jnp.bfloat16)
    outbound = spread.reshape(devices, capacity, model_width)
    block_in = lax.all_to_all(outbound, "seq", split_axis=0, concat_axis=0, tiled=True)
    row_block = block_in.reshape(-1, model_width)
    gate_val = jnp.dot(row_block, expert_gate[0], preferred_element_type=jnp.float32)
    up_val = jnp.dot(row_block, expert_up[0], preferred_element_type=jnp.float32)
    hidden = (jax.nn.silu(gate_val) * up_val).astype(jnp.bfloat16)
    result = jnp.dot(hidden, expert_down[0], preferred_element_type=jnp.float32).astype(
        jnp.bfloat16
    )
    inbound = lax.all_to_all(
        result.reshape(block_in.shape), "seq", split_axis=0, concat_axis=0, tiled=True
    )
    flat_back = inbound.reshape(devices * capacity, model_width)
    first_out = jnp.dot(pick_first, flat_back, preferred_element_type=jnp.float32)
    second_out = jnp.dot(pick_second, flat_back, preferred_element_type=jnp.float32)
    expert_mix = route_weight[:, 0:1] * first_out + route_weight[:, 1:2] * second_out
    return (updated_float + expert_mix).astype(jnp.bfloat16)


def solution(mesh):
    return jax.shard_map(
        shards,
        mesh=mesh,
        in_specs=(
            P(("batch", "seq"), None),
            P(("batch", "seq"), None),
            P(("batch", "seq"), None),
            P(("batch", "seq"), None),
            P(None, ("batch", "seq")),
            P(None, ("batch", "seq")),
            P(),
            P(),
            P("seq", None, None),
            P("seq", None, None),
            P("seq", None, None),
            P(("batch", "seq"), None),
            P(("batch", "seq"), None),
        ),
        out_specs=P(("batch", "seq"), None),
        check_vma=False,
    )
```
